256 devices in a mesh: row: 32 (over z, y_hi, core), col: 8 (over y_lo, x).
Axes of the slice: x: 4, y: 4 (y_hi: 2, y_lo: 2; y = y_hi * 2 + y_lo), z: 8, core: 2. Of those that a mesh axis runs over, the one named last changes fastest.
Arguments:
- inputs: bfloat16 [12288, 1024], P(('row', 'col')), may hold values from -24 to 24
- first_weight: bfloat16 [1024, 1024], replicated, may hold values from -0.1875 to 0.1875
- second_weight: bfloat16 [1024, 1024], replicated, may hold values from -0.1875 to 0.1875
- readout: bfloat16 [1024], replicated, may hold values from -0.1875 to 0.1875
- target: float32 [12288], P(('row', 'col')), may hold values from -6 to 6
- counts: int32 [12288], P(('row', 'col')), may hold values from 1 to 32, as said below
- views: int32 [12288], P(('row', 'col')), may hold values from 0 to 1999
Outputs:
- update: float32 [1024, 2048], P(('row', 'col'))
The draws below stay inside these ranges and needn't reach their ends.
Inputs may be any that keep to these rules, and one draw needn't show every extreme that they name: `counts`: number of samples taken along the ray.
All inputs are finite; a program needn't handle non-finite values.
Results may differ from the reference program's by a relative error of at most 0.008.
Values may be sent and summed in bfloat16 or wider, within the bound.
A program may use at most 128 MiB of HBM per device.

```python
import jax
import jax.numpy as jnp
from jax import lax

D = 1024
VIEWS = 2000
ITERS = 3
ROWS = 12288


def draw_counts(key, part):
    positions = jnp.arange(ROWS, dtype=jnp.int32)
    top = 9 + 24 * positions // ROWS
    return jax.random.randint(key, (ROWS,), 1, top + 1, dtype=jnp.int32)


def set_ends(result, rng, low, largest):
    place = [jax.random.randint(jax.random.fold_in(rng, axis), (), 0, length) for axis, length in enumerate(result.shape)]
    main_axis = result.shape.index(max(result.shape))
    neighbour = place[:main_axis] + [(place[main_axis] + 1) % result.shape[main_axis]] + place[main_axis + 1:]
    return result.at[tuple(place)].set(low).at[tuple(neighbour)].set(largest)


def with_spikes(drawn, rng, source, target, parts, factor):
    owner, partner = [(jnp.arange(drawn.shape[dim]) // (drawn.shape[dim] // parts)).reshape([-1 if axis == dim else 1 for axis in range(drawn.ndim)]) for dim in (source, target)]
    chosen = jax.random.permutation(rng, parts)[partner]
    strong = (owner == chosen) | (owner == (partner + parts // 2) % parts)
    return jnp.where(strong, factor * drawn, drawn)


def shard_levels(stream_key, dims, pieces, low, top_value):
    def one(dim, parts):
        draws = jax.random.uniform(jax.random.fold_in(jax.random.fold_in(stream_key, 6), dim), (parts,), jnp.float32, low / len(pieces), top_value / len(pieces))
        return jnp.repeat(jnp.exp(draws), dims[dim] // parts).reshape((-1,) + (1,) * (len(dims) - dim - 1))

    factor_of = one(*pieces[0])
    for cut in pieces[1:]:
        factor_of = factor_of * one(*cut)
    return factor_of


def centred(key, extent, scale, reach, cuts=(), kind=jnp.bfloat16):
    gain = shard_levels(key, extent, cuts, -0.22, 0.18) if cuts else 1.0
    entries = jax.random.normal(key, extent, jnp.float32) * scale * gain
    return jnp.minimum(jnp.maximum(entries, -reach), reach).astype(kind)


def heavy_noise(stream_key, extent, width, bound, shards, heavy, kind=jnp.bfloat16):
    drawn = width * jax.random.normal(stream_key, extent, jnp.float32)
    if shards:
        drawn = drawn * shard_levels(stream_key, extent, shards, -0.22, 0.18)
    return jnp.clip(with_spikes(drawn, jax.random.fold_in(stream_key, 3), *heavy), -bound, bound).astype(kind)


def setup_inputs(seed: int = 0) -> dict:
    keys = jax.random.split(jax.random.key(seed), 8)
    inputs = heavy_noise(keys[0], (ROWS, D), 1.0, 24.0, ((0, 256),), (0, 1, 256, 6.0))
    first_weight = centred(keys[1], (D, D), D ** -0.5, 0.1875)
    second_weight = centred(keys[2], (D, D), D ** -0.5, 0.1875)
    readout = centred(keys[3], (D,), D ** -0.5, 0.1875)
    target = centred(keys[4], (ROWS,), 1.0, 6.0, ((0, 256),), jnp.float32)
    counts = draw_counts(jax.random.fold_in(keys[7], 71), 0)
    views = set_ends(jax.random.randint(keys[6], (ROWS,), 0, VIEWS), jax.random.fold_in(keys[6], 1), 0, VIEWS - 1).astype(jnp.int32)
    return dict(inputs=inputs, first_weight=first_weight, second_weight=second_weight, readout=readout, target=target, counts=counts, views=views)


DAMP = 4.0
LEARN = 8.0
HIGH = lax.Precision.HIGHEST


def slope(value):
    sig = jax.nn.sigmoid(value)
    return sig * (1.0 + value * (1.0 - sig))


def ray_weight(counts, views):
    angle = (2.0 * jnp.pi / VIEWS) * views.astype(jnp.float32)
    return counts.astype(jnp.float32) / 16.0 * (1.0 + 0.5 * jnp.cos(angle))


def reference(inputs, first_weight, second_weight, readout, target, counts, views):
    weight_rows = ray_weight(counts, views)
    pre_first = jnp.dot(inputs, first_weight, preferred_element_type=jnp.float32)
    hidden = jax.nn.silu(pre_first).astype(jnp.bfloat16)
    pre_second = jnp.dot(hidden, second_weight, preferred_element_type=jnp.float32)
    readout_f = readout.astype(jnp.float32)
    signal = jnp.sum(jax.nn.silu(pre_second) * readout_f[None, :], axis=1)
    right = weight_rows * signal - target
    outer_grad = (weight_rows[:, None] * slope(pre_second) * readout_f[None, :]).astype(jnp.bfloat16)
    carried = lax.dot_general(outer_grad, second_weight, (((1,), (1,)), ((), ())), preferred_element_type=jnp.float32)
    inner_grad = (carried * slope(pre_first)).astype(jnp.bfloat16)
    in_f = inputs.astype(jnp.float32)
    hid_f = hidden.astype(jnp.float32)
    inner_f = inner_grad.astype(jnp.float32)
    outer_f = outer_grad.astype(jnp.float32)

    def apply(direction):
        first = jnp.dot(in_f.T, direction[:, None] * inner_f, precision=HIGH)
        second = jnp.dot(hid_f.T, direction[:, None] * outer_f, precision=HIGH)
        total = jnp.sum(jnp.dot(in_f, first, precision=HIGH) * inner_f, axis=1)
        total = total + jnp.sum(jnp.dot(hid_f, second, precision=HIGH) * outer_f, axis=1)
        return total + DAMP * direction

    solution = jnp.zeros_like(right)
    residual, direction = right, right
    norm_now = jnp.sum(residual * residual)
    for step in range(ITERS):
        image = apply(direction)
        alpha = norm_now / jnp.sum(direction * image)
        solution = solution + alpha * direction
        residual = residual - alpha * image
        norm_next = jnp.sum(residual * residual)
        direction = residual + (norm_next / norm_now) * direction
        norm_now = norm_next
    first = jnp.dot(in_f.T, solution[:, None] * inner_f, precision=HIGH)
    second = jnp.dot(hid_f.T, solution[:, None] * outer_f, precision=HIGH)
    return -LEARN * jnp.concatenate([first, second], axis=1)
```

```python
import functools

import jax
import jax.numpy as jnp
from jax import lax
from jax.experimental import pallas as pl
from jax.experimental.pallas import tpu as pltpu
from jax.sharding import Mesh
from jax.sharding import PartitionSpec as P

VIEWS = 2000
DAMP = 4.0
LEARN = 8.0
AXES = ("z", "yh", "core", "yl", "x")
MESH = pl.DeviceIdType.MESH
F32 = jnp.float32
BF16 = jnp.bfloat16
CHUNK = 48
HALF = 384
SET = 768
WIDE = 256
NT = (((1,), (1,)), ((), ()))


def dot(a, b):
    return jnp.dot(a, b, preferred_element_type=F32)


def dot_nt(a, b):
    return lax.dot_general(a, b, NT, preferred_element_type=F32)


def sigmoid(value):
    return 0.5 * jnp.tanh(0.5 * value) + 0.5


def twice(column):
    return jnp.concatenate([column, column], axis=1)


def total_of(value):
    return jnp.sum(jnp.sum(value, axis=1, keepdims=True), axis=0, keepdims=True)


def step_kernel(
    x_hbm, w1_hbm, w2_hbm, side_ref, readout_ref, out_ref,
    w1, w2, xpa, xpb, hp, op, ip, xl, hl, ol, il, slope1, kern,
    side_p, side_l, side_rows, wcol_p, tcol_p, wcol_l, tcol_l, sig,
    half_r, x_t, h_t, plane_buf, line_buf, out_send, out_recv,
    load_sem, a_send, a_recv, b_send, b_recv, z_send, z_recv,
    core_send, core_recv, sp_sems, sl_sems, plane_sems, line_sems, out_sems,
):
    z, yh, c, yl, x = (lax.axis_index(name) for name in AXES)
    y = yh * 2 + yl
    me_p = y * 4 + x
    me_l = c * 8 + z

    def at(xx=None, yy=None, zz=None, cc=None):
        xx = x if xx is None else lax.rem(xx, 4)
        yy = y if yy is None else lax.rem(yy, 4)
        zz = z if zz is None else lax.rem(zz, 8)
        cc = c if cc is None else cc
        return (zz, yy // 2, cc, lax.rem(yy, 2), xx)

    plane_peers = [at(xx=x + k % 4, yy=y + k // 4) for k in range(1, 16)]
    line_same = [at(zz=z + k) for k in range(1, 8)]
    line_peers = line_same + [at(zz=z + k, cc=1 - c) for k in range(8)]

    def send(src, dst, ssem, rsem, dev):
        copy = pltpu.make_async_remote_copy(
            src_ref=src, dst_ref=dst, send_sem=ssem, recv_sem=rsem,
            device_id=dev, device_id_type=MESH,
        )
        copy.start()
        return copy

    def rows(slot, count=1):
        return pl.ds(pl.multiple_of(slot * CHUNK, CHUNK), count * CHUNK)

    loads = [
        pltpu.make_async_copy(x_hbm.at[:, pl.ds(0, 512)], xpa.at[rows(me_p)], load_sem.at[0]),
        pltpu.make_async_copy(x_hbm.at[:, pl.ds(512, 512)], xpb.at[rows(me_p)], load_sem.at[1]),
        pltpu.make_async_copy(x_hbm, xl.at[c, rows(z)], load_sem.at[2]),
        pltpu.make_async_copy(w1_hbm, w1, load_sem.at[3]),
        pltpu.make_async_copy(w2_hbm, w2, load_sem.at[4]),
    ]
    for load in loads:
        load.start()

    barrier = pltpu.get_barrier_semaphore()
    for peer in plane_peers + line_peers:
        pl.semaphore_signal(barrier, inc=1, device_id=peer, device_id_type=MESH)
    pl.semaphore_wait(barrier, 30)
    for load in loads[:3]:
        load.wait()

    xn, xq = at(xx=x + 1), at(xx=x + 3)
    yn, yq = at(yy=y + 1), at(yy=y + 3)
    zn, zq = at(zz=z + 1), at(zz=z + 7)
    xm1, xp1 = lax.rem(x + 3, 4), lax.rem(x + 1, 4)
    ym1, yp1 = lax.rem(y + 3, 4), lax.rem(y + 1, 4)
    pending = []

    def pa(yy, xx):
        return rows(yy * 4 + xx)

    def go(ref, index, ssem, rsem, k, dev):
        copy = send(ref.at[index], ref.at[index], ssem.at[k], rsem.at[k], dev)
        pending.append(copy)
        return copy

    own = rows(me_p)
    a1 = [go(xpa, (own,), a_send, a_recv, 0, xn), go(xpa, (own,), a_send, a_recv, 1, xq)]
    b1 = [go(xpb, (own,), b_send, b_recv, 0, yn), go(xpb, (own,), b_send, b_recv, 1, yq)]
    z1 = [
        go(xl, (c, rows(z)), z_send, z_recv, 0, zn),
        go(xl, (c, rows(z)), z_send, z_recv, 1, zq),
    ]
    for k in range(15):
        send(side_ref, side_p.at[me_p], sp_sems.at[0], sp_sems.at[1], plane_peers[k])
    for k in range(7):
        send(side_ref, side_l.at[z], sl_sems.at[0], sl_sems.at[1], line_same[k])
    side_p[me_p] = side_ref[...]
    side_l[z] = side_ref[...]

    low, high = pl.ds(0, 256), pl.ds(256, 256)
    a1[0].wait_recv()
    a2 = [go(xpa, (pa(y, xm1), low), a_send, a_recv, 2, xn)]
    a1[1].wait_recv()
    a2 += [go(xpa, (pa(y, xp1), high), a_send, a_recv, 3, xq)]
    b1[0].wait_recv()
    b2 = [go(xpb, (pa(ym1, x), low), b_send, b_recv, 2, yn)]
    b1[1].wait_recv()
    b2 += [go(xpb, (pa(yp1, x), high), b_send, b_recv, 3, yq)]

    def ring(step, before):
        down, up = lax.rem(z + 8 - step, 8), lax.rem(z + step, 8)
        lanes = (slice(None), slice(None)) if step < 3 else (pl.ds(0, 512), pl.ds(512, 512))
        before[0].wait_recv()
        one = go(xl, (c, rows(down), lanes[0]), z_send, z_recv, 2 * step, zn)
        before[1].wait_recv()
        two = go(xl, (c, rows(up), lanes[1]), z_send, z_recv, 2 * step + 1, zq)
        return [one, two]

    z2 = ring(1, z1)
    for copy in a2:
        copy.wait_recv()
    line_y = (rows(y * 4, 4),)
    a3 = [go(xpa, line_y, a_send, a_recv, 4, yn), go(xpa, line_y, a_send, a_recv, 5, yq)]
    for copy in b2:
        copy.wait_recv()
    b3 = []
    for side, dev in ((0, xn), (1, xq)):
        b3.append([go(xpb, (pa(yy, x),), b_send, b_recv, 4 + 4 * side + yy, dev) for yy in range(4)])
    z3 = ring(2, z2)
    a3[0].wait_recv()
    a4 = [go(xpa, (rows(ym1 * 4, 2),), a_send, a_recv, 6, yn)]
    a3[1].wait_recv()
    a4 += [go(xpa, (rows(yp1 * 4 + 2, 2),), a_send, a_recv, 7, yq)]
    b4 = []
    for copy in b3[0]:
        copy.wait_recv()
    b4 += [go(xpb, (pa(yy, xm1),), b_send, b_recv, 12 + yy, xn) for yy in range(2)]
    for copy in b3[1]:
        copy.wait_recv()
    b4 += [go(xpb, (pa(yy, xp1),), b_send, b_recv, 12 + yy, xq) for yy in range(2, 4)]
    z4 = ring(3, z3)

    def many(ref, count, sems, which):
        view = ref.at[pl.ds(0, count)]
        pltpu.make_async_copy(view, view, sems.at[which]).wait()

    many(side_p, 15, sp_sems, 1)
    many(side_l, 7, sl_sems, 1)
    side_rows[...] = jnp.zeros_like(side_rows)
    side_rows[0:16, :] = side_p[:, 0, :]
    side_rows[16:32, :] = side_p[:, 1, :]
    side_rows[32:40, :] = side_l[:, 0, :]
    side_rows[40:48, :] = side_l[:, 1, :]
    turned = side_rows[...].T
    for s in range(16):
        place = pl.ds(s * CHUNK, CHUNK)
        wcol_p[place, :] = jnp.broadcast_to(turned[0:CHUNK, s : s + 1], (CHUNK, 128))
        tcol_p[place, :] = jnp.broadcast_to(turned[0:CHUNK, 16 + s : 17 + s], (CHUNK, 128))
    for s in range(8):
        place = pl.ds(s * CHUNK, CHUNK)
        wcol_l[place, :] = jnp.broadcast_to(turned[0:CHUNK, 32 + s : 33 + s], (CHUNK, 128))
        tcol_l[place, :] = jnp.broadcast_to(turned[0:CHUNK, 40 + s : 41 + s], (CHUNK, 128))
    loads[3].wait()
    loads[4].wait()

    def wide(n):
        return pl.ds(pl.multiple_of(n * WIDE, WIDE), WIDE)

    def forward(x_parts, h_ref, o_ref, i_ref, wcol, tcol, after):
        def first(n, carry):
            pre = sum(dot(part[...], w1[lo : lo + size, wide(n)]) for part, lo, size in x_parts)
            s = sigmoid(pre)
            h_ref[:, wide(n)] = (pre * s).astype(BF16)
            slope1[:, wide(n)] = s * (1.0 + pre * (1.0 - s))
            return carry

        lax.fori_loop(0, 4, first, 0)
        after(0)
        sig[...] = jnp.zeros_like(sig)

        def second(n, carry):
            pre = dot(h_ref[...], w2[:, wide(n)])
            s = sigmoid(pre)
            gain = readout_ref[0:1, wide(n)]
            parts = pre * s * gain
            sig[...] += parts[:, 0:128] + parts[:, 128:256]
            o_ref[:, wide(n)] = (twice(wcol[...]) * (s * (1.0 + pre * (1.0 - s))) * gain).astype(BF16)
            return carry

        lax.fori_loop(0, 4, second, 0)
        after(1)

        def third(n, carry):
            back = dot_nt(o_ref[...], w2[wide(n), :])
            i_ref[:, wide(n)] = (back * slope1[:, wide(n)]).astype(BF16)
            return carry

        lax.fori_loop(0, 4, third, 0)
        after(2)
        lane = lax.broadcasted_iota(jnp.int32, (128, 128), 1)
        found = []
        for b in range(3):
            place = pl.ds(b * 128, 128)
            term = sig[place, :] * wcol[place, :] - jnp.where(lane == 0, tcol[place, :], 0.0)
            found.append(jnp.sum(term.T, axis=0, keepdims=True))
        return found

    sub = lax.broadcasted_iota(jnp.int32, (8, 128), 0)

    def packed(lines, first=0):
        value = jnp.zeros((8, 128), F32)
        for k, line in enumerate(lines):
            value = jnp.where(sub == first + k, line, value)
        return value

    for copy in z4:
        copy.wait_recv()
    partner = at(cc=1 - c)
    core_copies = [send(xl.at[c], xl.at[c], core_send.at[0], core_recv.at[0], partner)]

    def share(k):
        ref = (hl, ol, il)[k]
        core_copies.append(send(ref.at[c], ref.at[c], core_send.at[1 + k], core_recv.at[1 + k], partner))

    found = forward([(xl.at[c], 0, 1024)], hl.at[c], ol.at[c], il.at[c], wcol_l, tcol_l, share)
    half_r[c] = packed(found, c * 3)
    core_copies.append(send(half_r.at[c], half_r.at[c], core_send.at[4], core_recv.at[4], partner))

    for copy in a4 + b4:
        copy.wait_recv()
    found = []
    for b in range(2):
        place = pl.ds(b * HALF, HALF)
        found += forward(
            [(xpa.at[place], 0, 512), (xpb.at[place], 512, 512)],
            hp.at[place], op.at[place], ip.at[place], wcol_p.at[place], tcol_p.at[place],
            lambda k: None,
        )
    r0p = packed(found)

    def gram(which):
        def block(n, carry):
            place = wide(n)
            one = dot_nt(xl[which, :, 0:512], xpa[place, :]) + dot_nt(xl[which, :, 512:1024], xpb[place, :])
            value = one * dot_nt(il[which], ip[place, :])
            value = value + dot_nt(hl[which], hp[place, :]) * dot_nt(ol[which], op[place, :])
            kern[which, :, place] = value
            return carry

        lax.fori_loop(0, 3, block, 0)

    gram(c)
    for copy in core_copies:
        copy.wait_recv()
    r0l = half_r[0] + half_r[1]
    gram(1 - c)

    def products(dp, dl):
        lines_l, sums = [], [None] * 6
        for b in range(6):
            part = kern.at[b // 3, pl.ds((b % 3) * 128, 128)]
            if dl is not None:
                col = jnp.broadcast_to(dl[b : b + 1, :], (128, 128)).T
            acc = None
            for t in range(6):
                tile = part[:, t * 128 : (t + 1) * 128]
                term = tile * dp[t : t + 1, :]
                acc = term if acc is None else acc + term
                if dl is not None:
                    down = jnp.sum((tile * col).reshape(16, 8, 128), axis=0)
                    sums[t] = down if sums[t] is None else sums[t] + down
            lines_l.append(jnp.sum(acc.T, axis=0, keepdims=True))
        lines_p = [jnp.sum(s, axis=0, keepdims=True) for s in sums] if dl is not None else []
        return lines_p, packed(lines_l)

    def start_plane(k, value):
        plane_buf[k, me_p] = value
        for peer in plane_peers:
            send(plane_buf.at[k, me_p], plane_buf.at[k, me_p], plane_sems.at[k, 0], plane_sems.at[k, 1], peer)

    def start_line(k, value):
        line_buf[k, me_l] = value
        for peer in line_peers:
            send(line_buf.at[k, me_l], line_buf.at[k, me_l], line_sems.at[k, 0], line_sems.at[k, 1], peer)

    def end_plane(k):
        many(plane_buf.at[k], 15, plane_sems.at[k], 1)
        return jnp.sum(plane_buf[k], axis=0)

    def end_line(k):
        many(line_buf.at[k], 15, line_sems.at[k], 1)
        return jnp.sum(line_buf[k], axis=0)

    def scalars(m, n):
        return [jnp.zeros((1, 128), F32)] * 6 + [jnp.broadcast_to(m, (1, 128)), jnp.broadcast_to(n, (1, 128))]

    lines_p, part_l = products(r0p, r0l)
    start_plane(0, packed(lines_p))
    start_line(0, part_l)
    mine = pl.ds(pl.multiple_of(z * 128, 128), 128)
    for b in range(6):
        place = pl.ds((b % 3) * 128, 128)
        x_t[:, b * 128 : (b + 1) * 128] = xl[b // 3, place, mine].astype(F32).T
        h_t[:, b * 128 : (b + 1) * 128] = hl[b // 3, place, mine].astype(F32).T
    w0p = end_plane(0) + DAMP * r0p
    w0l = end_line(0) + DAMP * r0l
    m0, m1 = total_of(r0l * r0l), total_of(r0l * w0l)
    lines_p, part_l = products(w0p, w0l)
    start_plane(1, packed(lines_p + scalars(m0, m1)[6:]))
    start_line(1, part_l)
    got = end_plane(1)
    u0p = got + DAMP * w0p
    u0l = end_line(1) + DAMP * w0l
    rr0, rw0 = got[6:7, :], got[7:8, :]
    al0 = rr0 / rw0
    r1l, w1l = r0l - al0 * w0l, w0l - al0 * u0l
    w1p = w0p - al0 * u0p
    m0, m1 = total_of(r1l * r1l), total_of(r1l * w1l)
    start_plane(2, packed(scalars(m0, m1)))
    _, part_l = products(w1p, None)
    start_line(2, part_l)
    got = end_plane(2)
    u1l = end_line(2) + DAMP * w1l
    rr1, rw1 = got[6:7, :], got[7:8, :]
    be0 = rr1 / rr0
    al1 = rr1 / (rw1 - be0 * rr1 / al0)
    d1 = r1l + be0 * r0l
    r2l = r1l - al1 * (w1l + be0 * w0l)
    w2l = w1l - al1 * (u1l + be0 * u0l)
    m0, m1 = total_of(r2l * r2l), total_of(r2l * w2l)
    start_plane(3, packed(scalars(m0, m1)))
    got = end_plane(3)
    rr2, rw2 = got[6:7, :], got[7:8, :]
    be1 = rr2 / rr1
    al2 = rr2 / (rw2 - be1 * rr2 / al1)
    sol = al0 * r0l + al1 * d1 + al2 * (r2l + be1 * d1)

    across = jnp.concatenate([sol[b : b + 1, :] for b in range(6)], axis=1)

    def summed(turned_ref, right):
        left = jnp.concatenate(
            [turned_ref[pl.ds(pl.multiple_of(c * 32 + 64 * k, 32), 32), :] for k in range(2)], axis=0
        )
        left = left * across
        coarse = left.astype(BF16)
        fine = (left - coarse.astype(F32)).astype(BF16)
        both = dot(jnp.concatenate([coarse, fine], axis=0), right[...].reshape(SET, 1024))
        return -LEARN * (both[0:64] + both[64:128])

    one = summed(x_t, il)
    two = summed(h_t, ol)
    sub_wide = lax.broadcasted_iota(jnp.int32, (8, 1024), 0)
    for e in range(8):
        f, s = one[8 * e : 8 * e + 8], two[8 * e : 8 * e + 8]
        out_send[2 * e] = jnp.where(sub_wide < 4, f, pltpu.roll(s, 4, 0)).astype(BF16)
        out_send[2 * e + 1] = jnp.where(sub_wide < 4, pltpu.roll(f, 4, 0), s).astype(BF16)
    for k in range(1, 16):
        dest = lax.rem(y + k // 4, 4) * 4 + lax.rem(x + k % 4, 4)
        send(out_send.at[dest], out_recv.at[me_p], out_sems.at[0], out_sems.at[1], plane_peers[k - 1])
    out_recv[me_p] = out_send[me_p]
    many(out_recv, 15, out_sems, 1)
    result = jnp.sum(out_recv[...].astype(F32), axis=0)
    out_ref[:, 0:1024] = result[0:4]
    out_ref[:, 1024:2048] = result[4:8]

    for copy in pending + core_copies:
        copy.wait_send()
    many(side_p, 15, sp_sems, 0)
    many(side_l, 7, sl_sems, 0)
    for k in range(4):
        many(plane_buf.at[k], 15, plane_sems.at[k], 0)
    for k in range(3):
        many(line_buf.at[k], 15, line_sems.at[k], 0)
    many(out_send, 15, out_sems, 0)


def shards(inputs, first_weight, second_weight, readout, target, counts, views):
    angle = (2.0 * jnp.pi / VIEWS) * views.astype(F32)
    weight_rows = counts.astype(F32) / 16.0 * (1.0 + 0.5 * jnp.cos(angle))
    side = jnp.pad(jnp.stack([weight_rows, target]), ((0, 6), (0, 128 - CHUNK)))
    vmem = pl.BlockSpec(memory_space=pltpu.VMEM)
    hbm = pl.BlockSpec(memory_space=pltpu.HBM)
    dma = pltpu.SemaphoreType.DMA
    return pl.pallas_call(
        step_kernel,
        out_shape=jax.ShapeDtypeStruct((4, 2048), F32),
        in_specs=[hbm, hbm, hbm, vmem, vmem],
        out_specs=vmem,
        scratch_shapes=[
            pltpu.VMEM((1024, 1024), BF16), pltpu.VMEM((1024, 1024), BF16),
            pltpu.VMEM((SET, 512), BF16), pltpu.VMEM((SET, 512), BF16),
            pltpu.VMEM((SET, 1024), BF16), pltpu.VMEM((SET, 1024), BF16), pltpu.VMEM((SET, 1024), BF16),
            pltpu.VMEM((2, HALF, 1024), BF16), pltpu.VMEM((2, HALF, 1024), BF16),
            pltpu.VMEM((2, HALF, 1024), BF16), pltpu.VMEM((2, HALF, 1024), BF16),
            pltpu.VMEM((HALF, 1024), F32), pltpu.VMEM((2, HALF, SET), F32),
            pltpu.VMEM((16, 8, 128), F32), pltpu.VMEM((8, 8, 128), F32), pltpu.VMEM((128, 128), F32),
            pltpu.VMEM((SET, 128), F32), pltpu.VMEM((SET, 128), F32),
            pltpu.VMEM((HALF, 128), F32), pltpu.VMEM((HALF, 128), F32), pltpu.VMEM((HALF, 128), F32),
            pltpu.VMEM((2, 8, 128), F32), pltpu.VMEM((128, SET), F32), pltpu.VMEM((128, SET), F32),
            pltpu.VMEM((4, 16, 8, 128), F32), pltpu.VMEM((3, 16, 8, 128), F32),
            pltpu.VMEM((16, 8, 1024), BF16), pltpu.VMEM((16, 8, 1024), BF16),
            dma((5,)), dma((8,)), dma((8,)), dma((16,)), dma((16,)), dma((8,)), dma((8,)),
            dma((5,)), dma((5,)), dma((2,)), dma((2,)), dma((4, 2)), dma((3, 2)), dma((2,)),
        ],
        compiler_params=pltpu.CompilerParams(
            collective_id=0, has_side_effects=True, vmem_limit_bytes=56 * 1024 * 1024
        ),
    )(inputs, first_weight, second_weight, side, readout.astype(F32).reshape(1, 1024))


def solution(mesh):
    split = Mesh(mesh.devices.reshape(8, 2, 2, 2, 4), AXES)
    return jax.shard_map(
        shards,
        mesh=split,
        in_specs=(P(AXES, None), P(), P(), P(), P(AXES), P(AXES), P(AXES)),
        out_specs=P(AXES, None),
        check_vma=False,
    )
```

```python
import functools

import jax
import jax.numpy as jnp
from jax import lax
from jax.experimental import pallas as pl
from jax.experimental.pallas import tpu as pltpu
from jax.sharding import Mesh
from jax.sharding import PartitionSpec as P

VIEWS = 2000
DAMP = 4.0
LEARN = 8.0
AXES = ("z", "yh", "core", "yl", "x")
MESH = pl.DeviceIdType.MESH
F32 = jnp.float32
BF16 = jnp.bfloat16
CHUNK = 48
HALF = 384
SET = 768
WIDE = 256
UNROLL = 4
NT = (((1,), (1,)), ((), ()))


def dot(a, b):
    return jnp.dot(a, b, preferred_element_type=F32)


def dot_nt(a, b):
    return lax.dot_general(a, b, NT, preferred_element_type=F32)


def sigmoid(value):
    return 0.5 * jnp.tanh(0.5 * value) + 0.5


def twice(column):
    return jnp.concatenate([column, column], axis=1)


def total_of(value):
    return jnp.sum(jnp.sum(value, axis=1, keepdims=True), axis=0, keepdims=True)


def step_kernel(
    x_hbm, w1_hbm, w2_hbm, gain_hbm, target_hbm, counts_hbm, views_hbm, out_ref,
    gain_in, target_in, counts_in, views_in, gain_row, side_ref,
    w1, w2, xpa, xpb, hp, op, ip, xl, hl, ol, il, slope_p, slope_l, kern,
    side_p, side_l, side_rows, wcol_p, tcol_p, wcol_l, tcol_l, sig,
    half_r, x_t, h_t, plane_buf, line_buf, out_send, out_recv,
    load_sem, a_send, a_recv, b_send, b_recv, z_send, z_recv,
    core_send, core_recv, sp_sems, sl_sems, plane_sems, line_sems, out_sems,
):
    z, yh, c, yl, x = (lax.axis_index(name) for name in AXES)
    y = yh * 2 + yl
    me_p = y * 4 + x
    me_l = c * 8 + z

    def at(xx=None, yy=None, zz=None, cc=None):
        xx = x if xx is None else lax.rem(xx, 4)
        yy = y if yy is None else lax.rem(yy, 4)
        zz = z if zz is None else lax.rem(zz, 8)
        cc = c if cc is None else cc
        return (zz, yy // 2, cc, lax.rem(yy, 2), xx)

    plane_peers = [at(xx=x + k % 4, yy=y + k // 4) for k in range(1, 16)]
    line_same = [at(zz=z + k) for k in range(1, 8)]
    line_peers = line_same + [at(zz=z + k, cc=1 - c) for k in range(8)]

    def send(src, dst, ssem, rsem, dev):
        copy = pltpu.make_async_remote_copy(
            src_ref=src, dst_ref=dst, send_sem=ssem, recv_sem=rsem,
            device_id=dev, device_id_type=MESH,
        )
        copy.start()
        return copy

    def rows(slot, count=1):
        return pl.ds(pl.multiple_of(slot * CHUNK, CHUNK), count * CHUNK)

    loads = [
        pltpu.make_async_copy(x_hbm.at[:, pl.ds(0, 512)], xpa.at[rows(me_p)], load_sem.at[0]),
        pltpu.make_async_copy(x_hbm.at[:, pl.ds(512, 512)], xpb.at[rows(me_p)], load_sem.at[1]),
        pltpu.make_async_copy(x_hbm, xl.at[c, rows(z)], load_sem.at[2]),
        pltpu.make_async_copy(counts_hbm, counts_in, load_sem.at[3]),
        pltpu.make_async_copy(views_hbm, views_in, load_sem.at[4]),
        pltpu.make_async_copy(target_hbm, target_in, load_sem.at[5]),
        pltpu.make_async_copy(gain_hbm, gain_in, load_sem.at[6]),
        pltpu.make_async_copy(w1_hbm, w1, load_sem.at[7]),
        pltpu.make_async_copy(w2_hbm, w2, load_sem.at[8]),
    ]
    for load in loads:
        load.start()

    barrier = pltpu.get_barrier_semaphore()
    for peer in plane_peers + line_peers:
        pl.semaphore_signal(barrier, inc=1, device_id=peer, device_id_type=MESH)
    for load in loads[:7]:
        load.wait()
    side_ref[...] = jnp.zeros_like(side_ref)
    angle = (2.0 * jnp.pi / VIEWS) * views_in[...].astype(F32)
    side_ref[0:1, 0:CHUNK] = counts_in[...].astype(F32) / 16.0 * (1.0 + 0.5 * jnp.cos(angle))
    side_ref[1:2, 0:CHUNK] = target_in[...]
    gain = gain_in[...].astype(F32)
    for k in range(8):
        gain_row[:, k * 128 : (k + 1) * 128] = gain[k : k + 1, :]
    pl.semaphore_wait(barrier, 30)

    xn, xq = at(xx=x + 1), at(xx=x + 3)
    yn, yq = at(yy=y + 1), at(yy=y + 3)
    zn, zq = at(zz=z + 1), at(zz=z + 7)
    pending = []

    def go(ref, index, ssem, rsem, k, dev):
        copy = send(ref.at[index], ref.at[index], ssem.at[k], rsem.at[k], dev)
        pending.append(copy)
        return copy

    low, high = pl.ds(0, 256), pl.ds(256, 256)
    offsets = (0, 3, 1, 2)

    class Spread:
        def __init__(self, ref, place, near, far, ssem, rsem):
            self.ref, self.place, self.near, self.far = ref, place, near, far
            self.sems, self.sent = (ssem, rsem), {}

        def go(self, k, d1, d2, dev, lanes=None):
            index = (rows(self.place(d1, d2)),) + (() if lanes is None else (lanes,))
            self.sent[k] = go(self.ref, index, *self.sems, k, dev)

        def arrived(self, *keys):
            for k in keys:
                self.sent[k].wait_recv()

        def second(self, j):
            for side in range(2):
                self.go(4 + 4 * side + j, offsets[j], 0, self.far[side])

        def step(self, k):
            if k == 0:
                self.go(0, 0, 0, self.near[0])
                self.go(1, 0, 0, self.near[1])
                self.second(0)
            elif k == 1:
                self.arrived(0)
                self.go(2, 3, 0, self.near[0], low)
                self.arrived(1)
                self.go(3, 1, 0, self.near[1], high)
                self.second(1)
                self.second(2)
            elif k == 2:
                self.arrived(4, 8)
                self.go(12, 0, 3, self.far[0])
            elif k == 3:
                self.arrived(2, 3)
                self.second(3)
            elif k == 4:
                self.arrived(5, 9)
                self.go(13, 3, 1, self.far[1])
                self.arrived(6, 10)
                self.go(14, 1, 1, self.far[1])
            elif k == 5:
                self.arrived(7, 11)
                self.go(15, 2, 3, self.far[0])
            else:
                self.arrived(12, 13, 14, 15)

    half_a = Spread(
        xpa, lambda d1, d2: lax.rem(y + d2, 4) * 4 + lax.rem(x + d1, 4), (xn, xq), (yn, yq), a_send, a_recv
    )
    half_b = Spread(
        xpb, lambda d1, d2: lax.rem(y + d1, 4) * 4 + lax.rem(x + d2, 4), (yn, yq), (xn, xq), b_send, b_recv
    )
    ring_sent = {}
    parts = (pl.ds(0, 512), pl.ds(512, 512))

    def ring(step, side, h):
        owner = lax.rem(z + (8 - step if side == 0 else step), 8)
        key = step * 4 + side * 2 + h
        ring_sent[key] = go(xl, (c, rows(owner), parts[h]), z_send, z_recv, key, (zn, zq)[side])

    def ring_step(step, h):
        for side in range(2):
            ring_sent[(step - 1) * 4 + side * 2 + h].wait_recv()
            if step < 3 or side == h:
                ring(step, side, h)

    half_a.step(0)
    half_b.step(0)
    for h in range(2):
        for side in range(2):
            ring(0, side, h)
    for k in range(15):
        send(side_ref, side_p.at[me_p], sp_sems.at[0], sp_sems.at[1], plane_peers[k])
    for k in range(7):
        send(side_ref, side_l.at[z], sl_sems.at[0], sl_sems.at[1], line_same[k])
    side_p[me_p] = side_ref[...]
    side_l[z] = side_ref[...]
    half_a.step(1)
    half_b.step(1)
    ring_step(1, 0)
    ring_step(1, 1)
    for k in (2, 3):
        half_a.step(k)
        half_b.step(k)
    ring_step(2, 0)
    ring_step(2, 1)
    for k in (4, 5):
        half_a.step(k)
        half_b.step(k)
    ring_step(3, 0)
    ring_step(3, 1)

    def many(ref, count, sems, which):
        view = ref.at[pl.ds(0, count)]
        pltpu.make_async_copy(view, view, sems.at[which]).wait()

    many(side_p, 15, sp_sems, 1)
    many(side_l, 7, sl_sems, 1)
    side_rows[...] = jnp.zeros_like(side_rows)
    side_rows[0:16, :] = side_p[:, 0, :]
    side_rows[16:32, :] = side_p[:, 1, :]
    side_rows[32:40, :] = side_l[:, 0, :]
    side_rows[40:48, :] = side_l[:, 1, :]
    turned = side_rows[...].T
    for s in range(16):
        place = pl.ds(s * CHUNK, CHUNK)
        wcol_p[place, :] = jnp.broadcast_to(turned[0:CHUNK, s : s + 1], (CHUNK, 128))
        tcol_p[place, :] = jnp.broadcast_to(turned[0:CHUNK, 16 + s : 17 + s], (CHUNK, 128))
    for s in range(8):
        place = pl.ds(s * CHUNK, CHUNK)
        wcol_l[place, :] = jnp.broadcast_to(turned[0:CHUNK, 32 + s : 33 + s], (CHUNK, 128))
        tcol_l[place, :] = jnp.broadcast_to(turned[0:CHUNK, 40 + s : 41 + s], (CHUNK, 128))
    loads[7].wait()
    loads[8].wait()

    def wide(n):
        return pl.ds(pl.multiple_of(n * WIDE, WIDE), WIDE)

    def first(x_parts, h_ref, slope_ref):
        def body(n, carry):
            pre = sum(dot(part[...], w1[lo : lo + size, wide(n)]) for part, lo, size in x_parts)
            s = sigmoid(pre)
            h_ref[:, wide(n)] = (pre * s).astype(BF16)
            slope_ref[:, wide(n)] = s * (1.0 + pre * (1.0 - s))
            return carry

        lax.fori_loop(0, 4, body, 0, unroll=UNROLL)

    def second(h_ref, o_ref, wcol, tcol):
        sig[...] = jnp.zeros_like(sig)

        def body(n, carry):
            pre = dot(h_ref[...], w2[:, wide(n)])
            s = sigmoid(pre)
            gain = gain_row[0:1, wide(n)]
            silu = pre * s * gain
            sig[...] += silu[:, 0:128] + silu[:, 128:256]
            o_ref[:, wide(n)] = (twice(wcol[...]) * (s * (1.0 + pre * (1.0 - s))) * gain).astype(BF16)
            return carry

        lax.fori_loop(0, 4, body, 0, unroll=UNROLL)
        lane = lax.broadcasted_iota(jnp.int32, (128, 128), 1)
        found = []
        for b in range(3):
            place = pl.ds(b * 128, 128)
            term = sig[place, :] * wcol[place, :] - jnp.where(lane == 0, tcol[place, :], 0.0)
            found.append(jnp.sum(term.T, axis=0, keepdims=True))
        return found

    def third(o_ref, i_ref, slope_ref):
        def body(n, carry):
            back = dot_nt(o_ref[...], w2[wide(n), :])
            i_ref[:, wide(n)] = (back * slope_ref[:, wide(n)]).astype(BF16)
            return carry

        lax.fori_loop(0, 4, body, 0, unroll=UNROLL)

    sub = lax.broadcasted_iota(jnp.int32, (8, 128), 0)

    def packed(lines, first=0):
        value = jnp.zeros((8, 128), F32)
        for k, line in enumerate(lines):
            value = jnp.where(sub == first + k, line, value)
        return value

    for key in (12, 15):
        ring_sent[key].wait_recv()
    partner = at(cc=1 - c)
    core_copies = []

    def share(k, ref):
        core_copies.append(send(ref.at[c], ref.at[c], core_send.at[k], core_recv.at[k], partner))

    share(0, xl)
    first([(xl.at[c], 0, 1024)], hl.at[c], slope_l)
    share(1, hl)
    half_a.step(6)
    half_b.step(6)
    blocks = [pl.ds(b * HALF, HALF) for b in range(2)]
    for b in blocks:
        first([(xpa.at[b], 0, 512), (xpb.at[b], 512, 512)], hp.at[b], slope_p.at[b])
    half_r[c] = packed(second(hl.at[c], ol.at[c], wcol_l, tcol_l), c * 3)
    share(2, ol)
    share(4, half_r)
    third(ol.at[c], il.at[c], slope_l)
    share(3, il)
    found = []
    for b in blocks:
        found += second(hp.at[b], op.at[b], wcol_p.at[b], tcol_p.at[b])
        third(op.at[b], ip.at[b], slope_p.at[b])
    r0p = packed(found)

    def gram(which):
        def block(n, carry):
            place = wide(n)
            one = dot_nt(xl[which, :, 0:512], xpa[place, :]) + dot_nt(xl[which, :, 512:1024], xpb[place, :])
            value = one * dot_nt(il[which], ip[place, :])
            value = value + dot_nt(hl[which], hp[place, :]) * dot_nt(ol[which], op[place, :])
            kern[which, :, place] = value
            return carry

        lax.fori_loop(0, 3, block, 0, unroll=3)

    gram(c)
    for copy in core_copies:
        copy.wait_recv()
    r0l = half_r[0] + half_r[1]
    gram(1 - c)

    def products(dp, dl):
        lines_l, sums = [], [None] * 6
        for b in range(6):
            part = kern.at[b // 3, pl.ds((b % 3) * 128, 128)]
            if dl is not None:
                col = jnp.broadcast_to(dl[b : b + 1, :], (128, 128)).T
            acc = None
            for t in range(6):
                tile = part[:, t * 128 : (t + 1) * 128]
                term = tile * dp[t : t + 1, :]
                acc = term if acc is None else acc + term
                if dl is not None:
                    down = jnp.sum((tile * col).reshape(16, 8, 128), axis=0)
                    sums[t] = down if sums[t] is None else sums[t] + down
            lines_l.append(jnp.sum(acc.T, axis=0, keepdims=True))
        lines_p = [jnp.sum(s, axis=0, keepdims=True) for s in sums] if dl is not None else []
        return lines_p, packed(lines_l)

    def start_plane(k, value):
        plane_buf[k, me_p] = value
        for peer in plane_peers:
            send(plane_buf.at[k, me_p], plane_buf.at[k, me_p], plane_sems.at[k, 0], plane_sems.at[k, 1], peer)

    def start_line(k, value):
        line_buf[k, me_l] = value
        for peer in line_peers:
            send(line_buf.at[k, me_l], line_buf.at[k, me_l], line_sems.at[k, 0], line_sems.at[k, 1], peer)

    def end_plane(k):
        many(plane_buf.at[k], 15, plane_sems.at[k], 1)
        return jnp.sum(plane_buf[k], axis=0)

    def end_line(k):
        many(line_buf.at[k], 15, line_sems.at[k], 1)
        return jnp.sum(line_buf[k], axis=0)

    def scalars(m, n):
        return [jnp.zeros((1, 128), F32)] * 6 + [jnp.broadcast_to(m, (1, 128)), jnp.broadcast_to(n, (1, 128))]

    lines_p, part_l = products(r0p, r0l)
    start_plane(0, packed(lines_p))
    start_line(0, part_l)
    mine = pl.ds(pl.multiple_of(z * 128, 128), 128)
    for b in range(6):
        place = pl.ds((b % 3) * 128, 128)
        x_t[:, b * 128 : (b + 1) * 128] = xl[b // 3, place, mine].astype(F32).T
        h_t[:, b * 128 : (b + 1) * 128] = hl[b // 3, place, mine].astype(F32).T
    w0p = end_plane(0) + DAMP * r0p
    w0l = end_line(0) + DAMP * r0l
    m0, m1 = total_of(r0l * r0l), total_of(r0l * w0l)
    lines_p, part_l = products(w0p, w0l)
    start_plane(1, packed(lines_p + scalars(m0, m1)[6:]))
    start_line(1, part_l)
    got = end_plane(1)
    u0p = got + DAMP * w0p
    u0l = end_line(1) + DAMP * w0l
    rr0, rw0 = got[6:7, :], got[7:8, :]
    al0 = rr0 / rw0
    r1l, w1l = r0l - al0 * w0l, w0l - al0 * u0l
    w1p = w0p - al0 * u0p
    m0, m1 = total_of(r1l * r1l), total_of(r1l * w1l)
    start_plane(2, packed(scalars(m0, m1)))
    _, part_l = products(w1p, None)
    start_line(2, part_l)
    got = end_plane(2)
    u1l = end_line(2) + DAMP * w1l
    rr1, rw1 = got[6:7, :], got[7:8, :]
    be0 = rr1 / rr0
    al1 = rr1 / (rw1 - be0 * rr1 / al0)
    d1 = r1l + be0 * r0l
    r2l = r1l - al1 * (w1l + be0 * w0l)
    w2l = w1l - al1 * (u1l + be0 * u0l)
    m0, m1 = total_of(r2l * r2l), total_of(r2l * w2l)
    start_plane(3, packed(scalars(m0, m1)))
    got = end_plane(3)
    rr2, rw2 = got[6:7, :], got[7:8, :]
    be1 = rr2 / rr1
    al2 = rr2 / (rw2 - be1 * rr2 / al1)
    sol = al0 * r0l + al1 * d1 + al2 * (r2l + be1 * d1)

    across = jnp.concatenate([sol[b : b + 1, :] for b in range(6)], axis=1)

    def summed(turned_ref, right):
        left = jnp.concatenate(
            [turned_ref[pl.ds(pl.multiple_of(c * 32 + 64 * k, 32), 32), :] for k in range(2)], axis=0
        )
        left = left * across
        coarse = left.astype(BF16)
        fine = (left - coarse.astype(F32)).astype(BF16)
        both = dot(jnp.concatenate([coarse, fine], axis=0), right[...].reshape(SET, 1024))
        return -LEARN * (both[0:64] + both[64:128])

    one = summed(x_t, il)
    two = summed(h_t, ol)
    sub_wide = lax.broadcasted_iota(jnp.int32, (8, 1024), 0)
    for e in range(8):
        f, s = one[8 * e : 8 * e + 8], two[8 * e : 8 * e + 8]
        out_send[2 * e] = jnp.where(sub_wide < 4, f, pltpu.roll(s, 4, 0)).astype(BF16)
        out_send[2 * e + 1] = jnp.where(sub_wide < 4, pltpu.roll(f, 4, 0), s).astype(BF16)
    for k in range(1, 16):
        dest = lax.rem(y + k // 4, 4) * 4 + lax.rem(x + k % 4, 4)
        send(out_send.at[dest], out_recv.at[me_p], out_sems.at[0], out_sems.at[1], plane_peers[k - 1])
    out_recv[me_p] = out_send[me_p]
    many(out_recv, 15, out_sems, 1)
    result = jnp.sum(out_recv[...].astype(F32), axis=0)
    out_ref[:, 0:1024] = result[0:4]
    out_ref[:, 1024:2048] = result[4:8]

    for copy in pending + core_copies:
        copy.wait_send()
    many(side_p, 15, sp_sems, 0)
    many(side_l, 7, sl_sems, 0)
    for k in range(4):
        many(plane_buf.at[k], 15, plane_sems.at[k], 0)
    for k in range(3):
        many(line_buf.at[k], 15, line_sems.at[k], 0)
    many(out_send, 15, out_sems, 0)


def shards(inputs, first_weight, second_weight, readout, target, counts, views):
    vmem = pl.BlockSpec(memory_space=pltpu.VMEM)
    hbm = pl.BlockSpec(memory_space=pltpu.HBM)
    dma = pltpu.SemaphoreType.DMA
    return pl.pallas_call(
        step_kernel,
        out_shape=jax.ShapeDtypeStruct((4, 2048), F32),
        in_specs=[hbm] * 7,
        out_specs=vmem,
        scratch_shapes=[
            pltpu.VMEM((8, 128), BF16), pltpu.VMEM((1, CHUNK), F32),
            pltpu.VMEM((1, CHUNK), jnp.int32), pltpu.VMEM((1, CHUNK), jnp.int32),
            pltpu.VMEM((1, 1024), F32), pltpu.VMEM((8, 128), F32),
            pltpu.VMEM((1024, 1024), BF16), pltpu.VMEM((1024, 1024), BF16),
            pltpu.VMEM((SET, 512), BF16), pltpu.VMEM((SET, 512), BF16),
            pltpu.VMEM((SET, 1024), BF16), pltpu.VMEM((SET, 1024), BF16), pltpu.VMEM((SET, 1024), BF16),
            pltpu.VMEM((2, HALF, 1024), BF16), pltpu.VMEM((2, HALF, 1024), BF16),
            pltpu.VMEM((2, HALF, 1024), BF16), pltpu.VMEM((2, HALF, 1024), BF16),
            pltpu.VMEM((SET, 1024), F32), pltpu.VMEM((HALF, 1024), F32), pltpu.VMEM((2, HALF, SET), F32),
            pltpu.VMEM((16, 8, 128), F32), pltpu.VMEM((8, 8, 128), F32), pltpu.VMEM((128, 128), F32),
            pltpu.VMEM((SET, 128), F32), pltpu.VMEM((SET, 128), F32),
            pltpu.VMEM((HALF, 128), F32), pltpu.VMEM((HALF, 128), F32), pltpu.VMEM((HALF, 128), F32),
            pltpu.VMEM((2, 8, 128), F32), pltpu.VMEM((128, SET), F32), pltpu.VMEM((128, SET), F32),
            pltpu.VMEM((4, 16, 8, 128), F32), pltpu.VMEM((3, 16, 8, 128), F32),
            pltpu.VMEM((16, 8, 1024), BF16), pltpu.VMEM((16, 8, 1024), BF16),
            dma((9,)), dma((16,)), dma((16,)), dma((16,)), dma((16,)), dma((16,)), dma((16,)),
            dma((5,)), dma((5,)), dma((2,)), dma((2,)), dma((4, 2)), dma((3, 2)), dma((2,)),
        ],
        compiler_params=pltpu.CompilerParams(
            collective_id=0, has_side_effects=True, vmem_limit_bytes=56 * 1024 * 1024
        ),
    )(
        inputs, first_weight, second_weight, readout.reshape(8, 128),
        target.reshape(1, CHUNK), counts.reshape(1, CHUNK), views.reshape(1, CHUNK),
    )


def solution(mesh):
    split = Mesh(mesh.devices.reshape(8, 2, 2, 2, 4), AXES)
    return jax.shard_map(
        shards,
        mesh=split,
        in_specs=(P(AXES, None), P(), P(), P(), P(AXES), P(AXES), P(AXES)),
        out_specs=P(AXES, None),
        check_vma=False,
    )
```

```python
import functools

import jax
import jax.numpy as jnp
from jax import lax
from jax.experimental import pallas as pl
from jax.experimental.pallas import tpu as pltpu
from jax.sharding import Mesh
from jax.sharding import PartitionSpec as P

VIEWS = 2000
DAMP = 4.0
LEARN = 8.0
AXES = ("z", "yh", "core", "yl", "x")
MESH = pl.DeviceIdType.MESH
F32 = jnp.float32
BF16 = jnp.bfloat16
CHUNK = 48
HALF = 384
SET = 768
WIDE = 256
NT = (((1,), (1,)), ((), ()))


def dot(a, b):
    return jnp.dot(a, b, preferred_element_type=F32)


def dot_nt(a, b):
    return lax.dot_general(a, b, NT, preferred_element_type=F32)


def sigmoid(value):
    return 0.5 * jnp.tanh(0.5 * value) + 0.5


def twice(column):
    return jnp.concatenate([column, column], axis=1)


def total_of(value):
    return jnp.sum(jnp.sum(value, axis=1, keepdims=True), axis=0, keepdims=True)


def step_kernel(
    x_hbm, w1_hbm, w2_hbm, gain_hbm, target_hbm, counts_hbm, views_hbm, out_ref,
    gain_in, target_in, counts_in, views_in, gain_row, side_ref,
    w1, w2, xpa, xpb, hp, op, ip, xl, hl, ol, il, xs, hs, os, slope, wcol, kern,
    side_p, side_l, side_rows, wcol_p, tcol_p, wcol_l, tcol_l, sig, q_p, q_l,
    half_r, x_t, h_t, plane_buf, line_buf, out_send, out_recv,
    load_sem, a_send, a_recv, b_send, b_recv, z_send, z_recv,
    core_send, core_recv, sp_sems, sl_sems, plane_sems, line_sems, out_sems,
):
    z, yh, c, yl, x = (lax.axis_index(name) for name in AXES)
    y = yh * 2 + yl
    me_p = y * 4 + x
    me_l = c * 8 + z

    def at(xx=None, yy=None, zz=None, cc=None):
        xx = x if xx is None else lax.rem(xx, 4)
        yy = y if yy is None else lax.rem(yy, 4)
        zz = z if zz is None else lax.rem(zz, 8)
        cc = c if cc is None else cc
        return (zz, yy // 2, cc, lax.rem(yy, 2), xx)

    plane_peers = [at(xx=x + k % 4, yy=y + k // 4) for k in range(1, 16)]
    line_same = [at(zz=z + k) for k in range(1, 8)]
    line_peers = line_same + [at(zz=z + k, cc=1 - c) for k in range(8)]

    def send(src, dst, ssem, rsem, dev):
        copy = pltpu.make_async_remote_copy(
            src_ref=src, dst_ref=dst, send_sem=ssem, recv_sem=rsem,
            device_id=dev, device_id_type=MESH,
        )
        copy.start()
        return copy

    def rows(slot, count=1):
        return pl.ds(pl.multiple_of(slot * CHUNK, CHUNK), count * CHUNK)

    loads = [
        pltpu.make_async_copy(x_hbm.at[:, pl.ds(0, 512)], xpa.at[rows(me_p)], load_sem.at[0]),
        pltpu.make_async_copy(x_hbm.at[:, pl.ds(512, 512)], xpb.at[rows(me_p)], load_sem.at[1]),
        pltpu.make_async_copy(x_hbm, xl.at[c, rows(z)], load_sem.at[2]),
        pltpu.make_async_copy(counts_hbm, counts_in, load_sem.at[3]),
        pltpu.make_async_copy(views_hbm, views_in, load_sem.at[4]),
        pltpu.make_async_copy(target_hbm, target_in, load_sem.at[5]),
        pltpu.make_async_copy(gain_hbm, gain_in, load_sem.at[6]),
        pltpu.make_async_copy(w1_hbm, w1, load_sem.at[7]),
        pltpu.make_async_copy(w2_hbm, w2, load_sem.at[8]),
    ]
    for load in loads:
        load.start()

    barrier = pltpu.get_barrier_semaphore()
    for peer in plane_peers + line_peers:
        pl.semaphore_signal(barrier, inc=1, device_id=peer, device_id_type=MESH)
    for load in loads[:7]:
        load.wait()
    side_ref[...] = jnp.zeros_like(side_ref)
    angle = (2.0 * jnp.pi / VIEWS) * views_in[...].astype(F32)
    side_ref[0:1, 0:CHUNK] = counts_in[...].astype(F32) / 16.0 * (1.0 + 0.5 * jnp.cos(angle))
    side_ref[1:2, 0:CHUNK] = target_in[...]
    gain = gain_in[...].astype(F32)
    for k in range(8):
        gain_row[:, k * 128 : (k + 1) * 128] = gain[k : k + 1, :]
    pl.semaphore_wait(barrier, 30)

    xn, xq = at(xx=x + 1), at(xx=x + 3)
    yn, yq = at(yy=y + 1), at(yy=y + 3)
    zn, zq = at(zz=z + 1), at(zz=z + 7)
    pending = []

    def go(ref, index, ssem, rsem, k, dev):
        copy = send(ref.at[index], ref.at[index], ssem.at[k], rsem.at[k], dev)
        pending.append(copy)
        return copy

    low, high = pl.ds(0, 256), pl.ds(256, 256)
    offsets = (0, 3, 1, 2)

    class Spread:
        def __init__(self, ref, place, near, far, ssem, rsem):
            self.ref, self.place, self.near, self.far = ref, place, near, far
            self.sems, self.sent = (ssem, rsem), {}

        def go(self, k, d1, d2, dev, lanes=None):
            index = (rows(self.place(d1, d2)),) + (() if lanes is None else (lanes,))
            self.sent[k] = go(self.ref, index, *self.sems, k, dev)

        def arrived(self, *keys):
            for k in keys:
                self.sent[k].wait_recv()

        def second(self, j):
            for side in range(2):
                self.go(4 + 4 * side + j, offsets[j], 0, self.far[side])

        def start(self):
            self.go(0, 0, 0, self.near[0])
            self.go(1, 0, 0, self.near[1])
            self.second(0)

        def hop(self, k):
            if k == 1:
                self.arrived(0)
                self.go(2, 3, 0, self.near[0], low)
                self.arrived(1)
                self.go(3, 1, 0, self.near[1], high)
                self.second(1)
                self.second(2)
                self.arrived(4, 8)
                self.go(12, 0, 3, self.far[0])
            elif k == 2:
                self.arrived(2, 3)
                self.second(3)
                self.arrived(5, 9)
                self.go(13, 3, 1, self.far[1])
                self.arrived(6, 10)
                self.go(14, 1, 1, self.far[1])
                self.arrived(12)
            elif k == 3:
                self.arrived(7, 11)
                self.go(15, 2, 3, self.far[0])
                self.arrived(13, 14)
            else:
                self.arrived(15)

    half_a = Spread(
        xpa, lambda d1, d2: lax.rem(y + d2, 4) * 4 + lax.rem(x + d1, 4), (xn, xq), (yn, yq), a_send, a_recv
    )
    half_b = Spread(
        xpb, lambda d1, d2: lax.rem(y + d1, 4) * 4 + lax.rem(x + d2, 4), (yn, yq), (xn, xq), b_send, b_recv
    )
    ring_sent = {}
    parts = (pl.ds(0, 512), pl.ds(512, 512))

    def ring(step, side, h):
        owner = lax.rem(z + (8 - step if side == 0 else step), 8)
        key = step * 4 + side * 2 + h
        ring_sent[key] = go(xl, (c, rows(owner), parts[h]), z_send, z_recv, key, (zn, zq)[side])

    def ring_step(step, h):
        for side in range(2):
            ring_sent[(step - 1) * 4 + side * 2 + h].wait_recv()
            if step < 3 or side == h:
                ring(step, side, h)

    for k in range(15):
        send(side_ref, side_p.at[me_p], sp_sems.at[0], sp_sems.at[1], plane_peers[k])
    for k in range(7):
        send(side_ref, side_l.at[z], sl_sems.at[0], sl_sems.at[1], line_same[k])
    half_a.start()
    half_b.start()
    for h in range(2):
        for side in range(2):
            ring(0, side, h)
    side_p[me_p] = side_ref[...]
    side_l[z] = side_ref[...]

    def hop(k):
        half_a.hop(k)
        half_b.hop(k)
        if k < 4:
            ring_step(k, 0)
            ring_step(k, 1)
        else:
            for key in (12, 15):
                ring_sent[key].wait_recv()

    near = {0: ((0, 0),), 1: ((0, 1), (0, 3), (1, 0), (3, 0)),
            2: ((2, 0), (0, 2), (1, 1), (1, 3), (3, 1), (3, 3)),
            3: ((2, 1), (2, 3), (1, 2), (3, 2)), 4: ((2, 2),)}

    def plane_slots(k):
        return [lax.rem(y + dy, 4) * 4 + lax.rem(x + dx, 4) for dx, dy in near[k]]

    def line_slots(k):
        return [lax.rem(z + d, 8) for d in ((k,) if k in (0, 4) else (k, 8 - k))]

    def many(ref, count, sems, which):
        view = ref.at[pl.ds(0, count)]
        pltpu.make_async_copy(view, view, sems.at[which]).wait()

    def columns():
        many(side_p, 15, sp_sems, 1)
        many(side_l, 7, sl_sems, 1)
        side_rows[...] = jnp.zeros_like(side_rows)
        side_rows[0:16, :] = side_p[:, 0, :]
        side_rows[16:32, :] = side_p[:, 1, :]
        side_rows[32:40, :] = side_l[:, 0, :]
        side_rows[40:48, :] = side_l[:, 1, :]
        turned = side_rows[...].T
        lane = lax.broadcasted_iota(jnp.int32, (CHUNK, 128), 1)
        for s in range(16):
            place = pl.ds(s * CHUNK, CHUNK)
            wcol_p[place, :] = jnp.broadcast_to(turned[0:CHUNK, s : s + 1], (CHUNK, 128))
            tcol_p[place, :] = jnp.where(lane == 0, turned[0:CHUNK, 16 + s : 17 + s], 0.0)
        for s in range(8):
            place = pl.ds(s * CHUNK, CHUNK)
            wcol_l[place, :] = jnp.broadcast_to(turned[0:CHUNK, 32 + s : 33 + s], (CHUNK, 128))
            tcol_l[place, :] = jnp.where(lane == 0, turned[0:CHUNK, 40 + s : 41 + s], 0.0)

    def wide(n):
        return pl.ds(pl.multiple_of(n * WIDE, WIDE), WIDE)

    def batch(line, plane, middle):
        chunks = [(xl, hl, ol, il, q_l, wcol_l, tcol_l, slot) for slot in line]
        chunks += [(None, hp, op, ip, q_p, wcol_p, tcol_p, slot) for slot in plane]
        size = len(chunks) * CHUNK
        span = pl.ds(0, size)
        for k, chunk in enumerate(chunks):
            to, at_slot = pl.ds(k * CHUNK, CHUNK), rows(chunk[-1])
            if chunk[0] is None:
                xs[to, 0:512] = xpa[at_slot, :]
                xs[to, 512:1024] = xpb[at_slot, :]
            else:
                xs[to, :] = xl[c, at_slot, :]

        def put(which, lanes, value):
            for k, chunk in enumerate(chunks):
                piece = value[k * CHUNK : (k + 1) * CHUNK]
                if chunk[0] is None:
                    chunk[which][rows(chunk[-1]), lanes] = piece
                else:
                    chunk[which][c, rows(chunk[-1]), lanes] = piece

        for n in range(4):
            lanes = pl.ds(n * WIDE, WIDE)
            pre = dot(xs[span, :], w1[:, lanes])
            s = sigmoid(pre)
            value = (pre * s).astype(BF16)
            hs[span, lanes] = value
            put(1, lanes, value)
            slope[span, lanes] = s * (1.0 + pre * (1.0 - s))
        middle()
        for k, chunk in enumerate(chunks):
            to, at_slot = pl.ds(k * CHUNK, CHUNK), rows(chunk[-1])
            wcol[to, :] = chunk[5][at_slot, :]
        for n in range(4):
            lanes = pl.ds(n * WIDE, WIDE)
            pre = dot(hs[span, :], w2[:, lanes])
            s = sigmoid(pre)
            gain = gain_row[0:1, lanes]
            silu = pre * s * gain
            silu = silu[:, 0:128] + silu[:, 128:256]
            if n == 0:
                sig[span, :] = silu
            else:
                sig[span, :] += silu
            value = (twice(wcol[span, :]) * (s * (1.0 + pre * (1.0 - s))) * gain).astype(BF16)
            os[span, lanes] = value
            put(2, lanes, value)
        for n in range(4):
            lanes = pl.ds(n * WIDE, WIDE)
            back = dot_nt(os[span, :], w2[lanes, :])
            put(3, lanes, (back * slope[span, lanes]).astype(BF16))
        for k, chunk in enumerate(chunks):
            to, at_slot = pl.ds(k * CHUNK, CHUNK), rows(chunk[-1])
            chunk[4][at_slot, :] = sig[to, :] * wcol[to, :] - chunk[6][at_slot, :]
        for slot in line:
            for ref in (xl, hl, ol, il):
                share(ref.at[c, rows(slot)])

    sub = lax.broadcasted_iota(jnp.int32, (8, 128), 0)

    def packed(lines, first=0):
        value = jnp.zeros((8, 128), F32)
        for k, line in enumerate(lines):
            value = jnp.where(sub == first + k, line, value)
        return value

    partner = at(cc=1 - c)
    core_copies = []

    def share(view):
        k = len(core_copies)
        core_copies.append(send(view, view, core_send.at[k], core_recv.at[k], partner))

    loads[7].wait()
    hop(1)
    loads[8].wait()
    batch(line_slots(0) + line_slots(1), plane_slots(0) + plane_slots(1), columns)
    for k in (2, 3, 4):
        hop(k)
        batch(line_slots(k), plane_slots(k), lambda: None)

    def as_lines(ref, count):
        return [jnp.sum(ref[pl.ds(b * 128, 128), :].T, axis=0, keepdims=True) for b in range(count)]

    half_r[c] = packed(as_lines(q_l, 3), c * 3)
    share(half_r.at[c])
    r0p = packed(as_lines(q_p, 6))

    def gram(which):
        def block(n, carry):
            place = wide(n)
            one = dot_nt(xl[which, :, 0:512], xpa[place, :]) + dot_nt(xl[which, :, 512:1024], xpb[place, :])
            value = one * dot_nt(il[which], ip[place, :])
            value = value + dot_nt(hl[which], hp[place, :]) * dot_nt(ol[which], op[place, :])
            kern[which, :, place] = value
            return carry

        lax.fori_loop(0, 3, block, 0, unroll=3)

    gram(c)
    for copy in core_copies:
        copy.wait_recv()
    r0l = half_r[0] + half_r[1]
    gram(1 - c)

    def products(dp, dl):
        lines_l, sums = [], [None] * 6
        for b in range(6):
            part = kern.at[b // 3, pl.ds((b % 3) * 128, 128)]
            if dl is not None:
                col = jnp.broadcast_to(dl[b : b + 1, :], (128, 128)).T
            acc = None
            for t in range(6):
                tile = part[:, t * 128 : (t + 1) * 128]
                term = tile * dp[t : t + 1, :]
                acc = term if acc is None else acc + term
                if dl is not None:
                    down = jnp.sum((tile * col).reshape(16, 8, 128), axis=0)
                    sums[t] = down if sums[t] is None else sums[t] + down
            lines_l.append(jnp.sum(acc.T, axis=0, keepdims=True))
        lines_p = [jnp.sum(s, axis=0, keepdims=True) for s in sums] if dl is not None else []
        return lines_p, packed(lines_l)

    def start_plane(k, value):
        plane_buf[k, me_p] = value
        for peer in plane_peers:
            send(plane_buf.at[k, me_p], plane_buf.at[k, me_p], plane_sems.at[k, 0], plane_sems.at[k, 1], peer)

    def start_line(k, value):
        line_buf[k, me_l] = value
        for peer in line_peers:
            send(line_buf.at[k, me_l], line_buf.at[k, me_l], line_sems.at[k, 0], line_sems.at[k, 1], peer)

    def end_plane(k):
        many(plane_buf.at[k], 15, plane_sems.at[k], 1)
        return jnp.sum(plane_buf[k], axis=0)

    def end_line(k):
        many(line_buf.at[k], 15, line_sems.at[k], 1)
        return jnp.sum(line_buf[k], axis=0)

    def scalars(m, n):
        return [jnp.zeros((1, 128), F32)] * 6 + [jnp.broadcast_to(m, (1, 128)), jnp.broadcast_to(n, (1, 128))]

    lines_p, part_l = products(r0p, r0l)
    start_plane(0, packed(lines_p))
    start_line(0, part_l)
    mine = pl.ds(pl.multiple_of(z * 128, 128), 128)
    for b in range(6):
        place = pl.ds((b % 3) * 128, 128)
        x_t[:, b * 128 : (b + 1) * 128] = xl[b // 3, place, mine].astype(F32).T
        h_t[:, b * 128 : (b + 1) * 128] = hl[b // 3, place, mine].astype(F32).T
    w0p = end_plane(0) + DAMP * r0p
    w0l = end_line(0) + DAMP * r0l
    m0, m1 = total_of(r0l * r0l), total_of(r0l * w0l)
    lines_p, part_l = products(w0p, w0l)
    start_plane(1, packed(lines_p + scalars(m0, m1)[6:]))
    start_line(1, part_l)
    got = end_plane(1)
    u0p = got + DAMP * w0p
    u0l = end_line(1) + DAMP * w0l
    rr0, rw0 = got[6:7, :], got[7:8, :]
    al0 = rr0 / rw0
    r1l, w1l = r0l - al0 * w0l, w0l - al0 * u0l
    w1p = w0p - al0 * u0p
    m0, m1 = total_of(r1l * r1l), total_of(r1l * w1l)
    start_plane(2, packed(scalars(m0, m1)))
    _, part_l = products(w1p, None)
    start_line(2, part_l)
    got = end_plane(2)
    u1l = end_line(2) + DAMP * w1l
    rr1, rw1 = got[6:7, :], got[7:8, :]
    be0 = rr1 / rr0
    al1 = rr1 / (rw1 - be0 * rr1 / al0)
    d1 = r1l + be0 * r0l
    r2l = r1l - al1 * (w1l + be0 * w0l)
    w2l = w1l - al1 * (u1l + be0 * u0l)
    m0, m1 = total_of(r2l * r2l), total_of(r2l * w2l)
    start_plane(3, packed(scalars(m0, m1)))
    got = end_plane(3)
    rr2, rw2 = got[6:7, :], got[7:8, :]
    be1 = rr2 / rr1
    al2 = rr2 / (rw2 - be1 * rr2 / al1)
    sol = al0 * r0l + al1 * d1 + al2 * (r2l + be1 * d1)

    across = jnp.concatenate([sol[b : b + 1, :] for b in range(6)], axis=1)

    def summed(turned_ref, right):
        left = jnp.concatenate(
            [turned_ref[pl.ds(pl.multiple_of(c * 32 + 64 * k, 32), 32), :] for k in range(2)], axis=0
        )
        left = left * across
        coarse = left.astype(BF16)
        fine = (left - coarse.astype(F32)).astype(BF16)
        both = dot(jnp.concatenate([coarse, fine], axis=0), right[...].reshape(SET, 1024))
        return -LEARN * (both[0:64] + both[64:128])

    one = summed(x_t, il)
    two = summed(h_t, ol)
    sub_wide = lax.broadcasted_iota(jnp.int32, (8, 1024), 0)
    for e in range(8):
        f, s = one[8 * e : 8 * e + 8], two[8 * e : 8 * e + 8]
        out_send[2 * e] = jnp.where(sub_wide < 4, f, pltpu.roll(s, 4, 0)).astype(BF16)
        out_send[2 * e + 1] = jnp.where(sub_wide < 4, pltpu.roll(f, 4, 0), s).astype(BF16)
    for k in range(1, 16):
        dest = lax.rem(y + k // 4, 4) * 4 + lax.rem(x + k % 4, 4)
        send(out_send.at[dest], out_recv.at[me_p], out_sems.at[0], out_sems.at[1], plane_peers[k - 1])
    out_recv[me_p] = out_send[me_p]
    many(out_recv, 15, out_sems, 1)
    result = jnp.sum(out_recv[...].astype(F32), axis=0)
    out_ref[:, 0:1024] = result[0:4]
    out_ref[:, 1024:2048] = result[4:8]

    for copy in pending + core_copies:
        copy.wait_send()
    many(side_p, 15, sp_sems, 0)
    many(side_l, 7, sl_sems, 0)
    for k in range(4):
        many(plane_buf.at[k], 15, plane_sems.at[k], 0)
    for k in range(3):
        many(line_buf.at[k], 15, line_sems.at[k], 0)
    many(out_send, 15, out_sems, 0)


def shards(inputs, first_weight, second_weight, readout, target, counts, views):
    vmem = pl.BlockSpec(memory_space=pltpu.VMEM)
    hbm = pl.BlockSpec(memory_space=pltpu.HBM)
    dma = pltpu.SemaphoreType.DMA
    return pl.pallas_call(
        step_kernel,
        out_shape=jax.ShapeDtypeStruct((4, 2048), F32),
        in_specs=[hbm] * 7,
        out_specs=vmem,
        scratch_shapes=[
            pltpu.VMEM((8, 128), BF16), pltpu.VMEM((1, CHUNK), F32),
            pltpu.VMEM((1, CHUNK), jnp.int32), pltpu.VMEM((1, CHUNK), jnp.int32),
            pltpu.VMEM((1, 1024), F32), pltpu.VMEM((2, 128), F32),
            pltpu.VMEM((1024, 1024), BF16), pltpu.VMEM((1024, 1024), BF16),
            pltpu.VMEM((SET, 512), BF16), pltpu.VMEM((SET, 512), BF16),
            pltpu.VMEM((SET, 1024), BF16), pltpu.VMEM((SET, 1024), BF16), pltpu.VMEM((SET, 1024), BF16),
            pltpu.VMEM((2, HALF, 1024), BF16), pltpu.VMEM((2, HALF, 1024), BF16),
            pltpu.VMEM((2, HALF, 1024), BF16), pltpu.VMEM((2, HALF, 1024), BF16),
            pltpu.VMEM((HALF, 1024), BF16), pltpu.VMEM((HALF, 1024), BF16), pltpu.VMEM((HALF, 1024), BF16),
            pltpu.VMEM((HALF, 1024), F32), pltpu.VMEM((HALF, 128), F32),
            pltpu.VMEM((2, HALF, SET), F32),
            pltpu.VMEM((16, 2, 128), F32), pltpu.VMEM((8, 2, 128), F32), pltpu.VMEM((128, 128), F32),
            pltpu.VMEM((SET, 128), F32), pltpu.VMEM((SET, 128), F32),
            pltpu.VMEM((HALF, 128), F32), pltpu.VMEM((HALF, 128), F32), pltpu.VMEM((HALF, 128), F32),
            pltpu.VMEM((SET, 128), F32), pltpu.VMEM((HALF, 128), F32),
            pltpu.VMEM((2, 8, 128), F32), pltpu.VMEM((128, SET), F32), pltpu.VMEM((128, SET), F32),
            pltpu.VMEM((4, 16, 8, 128), F32), pltpu.VMEM((3, 16, 8, 128), F32),
            pltpu.VMEM((16, 8, 1024), BF16), pltpu.VMEM((16, 8, 1024), BF16),
            dma((9,)), dma((16,)), dma((16,)), dma((16,)), dma((16,)), dma((16,)), dma((16,)),
            dma((33,)), dma((33,)), dma((2,)), dma((2,)), dma((4, 2)), dma((3, 2)), dma((2,)),
        ],
        compiler_params=pltpu.CompilerParams(
            collective_id=0, has_side_effects=True, vmem_limit_bytes=56 * 1024 * 1024
        ),
    )(
        inputs, first_weight, second_weight, readout.reshape(8, 128),
        target.reshape(1, CHUNK), counts.reshape(1, CHUNK), views.reshape(1, CHUNK),
    )


def solution(mesh):
    split = Mesh(mesh.devices.reshape(8, 2, 2, 2, 4), AXES)
    return jax.shard_map(
        shards,
        mesh=split,
        in_specs=(P(AXES, None), P(), P(), P(), P(AXES), P(AXES), P(AXES)),
        out_specs=P(AXES, None),
        check_vma=False,
    )
```

```python
import functools

import jax
import jax.numpy as jnp
from jax import lax
from jax.experimental import pallas as pl
from jax.experimental.pallas import tpu as pltpu
from jax.sharding import Mesh
from jax.sharding import PartitionSpec as P

VIEWS = 2000
DAMP = 4.0
LEARN = 8.0
AXES = ("z", "yh", "core", "yl", "x")
MESH = pl.DeviceIdType.MESH
F32 = jnp.float32
BF16 = jnp.bfloat16
CHUNK = 48
HALF = 384
SET = 768
WIDE = 256
NT = (((1,), (1,)), ((), ()))


def dot(a, b):
    return jnp.dot(a, b, preferred_element_type=F32)


def dot_nt(a, b):
    return lax.dot_general(a, b, NT, preferred_element_type=F32)


def sigmoid(value):
    return 0.5 * jnp.tanh(0.5 * value) + 0.5


def twice(column):
    return jnp.concatenate([column, column], axis=1)


def total_of(value):
    return jnp.sum(jnp.sum(value, axis=1, keepdims=True), axis=0, keepdims=True)


def step_kernel(
    x_hbm, w1_hbm, w2_hbm, gain_hbm, target_hbm, counts_hbm, views_hbm, out_ref,
    gain_in, target_in, counts_in, views_in, gain_row, side_ref,
    w1, w2, xpa, xpb, hp, op, ip, xl, hl, ol, il, xs, hs, os, slope, wcol, kern,
    side_p, side_l, side_rows, wcol_p, tcol_p, wcol_l, tcol_l, sig, q_p, q_l,
    half_r, x_t, h_t, terms, plane_buf, line_buf, out_send, out_recv,
    load_sem, a_send, a_recv, b_send, b_recv, z_send, z_recv,
    core_send, core_recv, sp_sems, sl_sems, plane_sems, line_sems, out_sems,
):
    z, yh, c, yl, x = (lax.axis_index(name) for name in AXES)
    y = yh * 2 + yl
    me_p = y * 4 + x
    me_l = c * 8 + z

    def at(xx=None, yy=None, zz=None, cc=None):
        xx = x if xx is None else lax.rem(xx, 4)
        yy = y if yy is None else lax.rem(yy, 4)
        zz = z if zz is None else lax.rem(zz, 8)
        cc = c if cc is None else cc
        return (zz, yy // 2, cc, lax.rem(yy, 2), xx)

    plane_order = (10, 6, 14, 9, 11, 2, 8, 5, 7, 13, 15, 1, 3, 4, 12)
    line_order = (4, 3, 5, 2, 6, 1, 7)
    plane_peers = [at(xx=x + k % 4, yy=y + k // 4) for k in plane_order]
    line_same = [at(zz=z + k) for k in line_order]
    line_peers = [at(zz=z + k, cc=c if q == 0 else 1 - c) for k in line_order for q in range(2)] + [at(cc=1 - c)]

    def send(src, dst, ssem, rsem, dev):
        copy = pltpu.make_async_remote_copy(
            src_ref=src, dst_ref=dst, send_sem=ssem, recv_sem=rsem,
            device_id=dev, device_id_type=MESH,
        )
        copy.start()
        return copy

    def rows(slot, count=1):
        return pl.ds(pl.multiple_of(slot * CHUNK, CHUNK), count * CHUNK)

    loads = [
        pltpu.make_async_copy(x_hbm.at[:, pl.ds(0, 512)], xpa.at[rows(me_p)], load_sem.at[0]),
        pltpu.make_async_copy(x_hbm.at[:, pl.ds(512, 512)], xpb.at[rows(me_p)], load_sem.at[1]),
        pltpu.make_async_copy(x_hbm, xl.at[c, rows(z)], load_sem.at[2]),
        pltpu.make_async_copy(counts_hbm, counts_in, load_sem.at[3]),
        pltpu.make_async_copy(views_hbm, views_in, load_sem.at[4]),
        pltpu.make_async_copy(target_hbm, target_in, load_sem.at[5]),
        pltpu.make_async_copy(gain_hbm, gain_in, load_sem.at[6]),
        pltpu.make_async_copy(w1_hbm, w1, load_sem.at[7]),
        pltpu.make_async_copy(w2_hbm, w2, load_sem.at[8]),
    ]
    for load in loads:
        load.start()

    barrier = pltpu.get_barrier_semaphore()
    for peer in plane_peers + line_peers:
        pl.semaphore_signal(barrier, inc=1, device_id=peer, device_id_type=MESH)
    for load in loads[:7]:
        load.wait()
    side_ref[...] = jnp.zeros_like(side_ref)
    angle = (2.0 * jnp.pi / VIEWS) * views_in[...].astype(F32)
    side_ref[0:1, 0:CHUNK] = counts_in[...].astype(F32) / 16.0 * (1.0 + 0.5 * jnp.cos(angle))
    side_ref[1:2, 0:CHUNK] = target_in[...]
    gain = gain_in[...].astype(F32)
    for k in range(8):
        gain_row[:, k * 128 : (k + 1) * 128] = gain[k : k + 1, :]
    pl.semaphore_wait(barrier, 30)

    xn, xq = at(xx=x + 1), at(xx=x + 3)
    yn, yq = at(yy=y + 1), at(yy=y + 3)
    zn, zq = at(zz=z + 1), at(zz=z + 7)
    pending = []

    def go(ref, index, ssem, rsem, k, dev):
        copy = send(ref.at[index], ref.at[index], ssem.at[k], rsem.at[k], dev)
        pending.append(copy)
        return copy

    low, high = pl.ds(0, 256), pl.ds(256, 256)
    offsets = (0, 3, 1, 2)

    class Spread:
        def __init__(self, ref, place, near, far, ssem, rsem):
            self.ref, self.place, self.near, self.far = ref, place, near, far
            self.sems, self.sent = (ssem, rsem), {}

        def go(self, k, d1, d2, dev, lanes=None):
            index = (rows(self.place(d1, d2)),) + (() if lanes is None else (lanes,))
            self.sent[k] = go(self.ref, index, *self.sems, k, dev)

        def arrived(self, *keys):
            for k in keys:
                self.sent[k].wait_recv()

        def second(self, j):
            for side in range(2):
                self.go(4 + 4 * side + j, offsets[j], 0, self.far[side])

        def start(self):
            self.go(0, 0, 0, self.near[0])
            self.go(1, 0, 0, self.near[1])
            self.second(0)

        def hop(self, k):
            if k == 1:
                self.arrived(0)
                self.go(2, 3, 0, self.near[0], low)
                self.arrived(1)
                self.go(3, 1, 0, self.near[1], high)
                self.second(1)
                self.second(2)
                self.arrived(4, 8)
                self.go(12, 0, 3, self.far[0])
            elif k == 2:
                self.arrived(2, 3)
                self.second(3)
                self.go(15, 2, 0, self.far[2])
                self.arrived(5, 9)
                self.go(13, 3, 1, self.far[1])
                self.arrived(6, 10)
                self.go(14, 1, 1, self.far[1])
                self.arrived(12)
            else:
                self.arrived(7, 11, 13, 14, 15)

    half_a = Spread(
        xpa, lambda d1, d2: lax.rem(y + d2, 4) * 4 + lax.rem(x + d1, 4), (xn, xq), (yn, yq, at(yy=y + 2)), a_send, a_recv
    )
    half_b = Spread(
        xpb, lambda d1, d2: lax.rem(y + d1, 4) * 4 + lax.rem(x + d2, 4), (yn, yq), (xn, xq, at(xx=x + 2)), b_send, b_recv
    )
    ring_sent = {}
    parts = (pl.ds(0, 512), pl.ds(512, 512))

    def ring(step, side, h, dist, dev):
        owner = lax.rem(z + (8 - dist if side == 0 else dist), 8)
        key = step * 4 + side * 2 + h
        ring_sent[key] = go(xl, (c, rows(owner), parts[h]), z_send, z_recv, key, dev)

    def ring_hop(k, h):
        for side in range(2):
            ring_sent[(k - 1) * 4 + side * 2 + h].wait_recv()
            if k < 3:
                ring(k, side, h, k, (zn, zq)[side])
            if k == 2 and side == h:
                ring(3, side, h, k, (at(zz=z + 2), at(zz=z + 6))[side])
        if k == 3 and h == 1:
            for key in (12, 15):
                ring_sent[key].wait_recv()

    half_a.start()
    half_b.start()
    for h in range(2):
        for side in range(2):
            ring(0, side, h, 0, (zn, zq)[side])
    for k in range(15):
        send(side_ref, side_p.at[me_p], sp_sems.at[0], sp_sems.at[1], plane_peers[k])
    for k in range(7):
        send(side_ref, side_l.at[z], sl_sems.at[0], sl_sems.at[1], line_same[k])
    side_p[me_p] = side_ref[...]
    side_l[z] = side_ref[...]

    def hop(k):
        ring_hop(k, 0)
        half_a.hop(k)
        ring_hop(k, 1)
        half_b.hop(k)

    near = {0: ((0, 0),), 1: ((0, 1), (0, 3), (1, 0), (3, 0)),
            2: ((2, 0), (0, 2), (1, 1), (1, 3), (3, 1), (3, 3)),
            3: ((2, 1), (2, 3), (1, 2), (3, 2), (2, 2))}

    def plane_slots(k):
        return [lax.rem(y + dy, 4) * 4 + lax.rem(x + dx, 4) for dx, dy in near[k]]

    def line_slots(k):
        return [lax.rem(z + d, 8) for d in {0: (0,), 1: (1, 7), 2: (2, 6), 3: (3, 5, 4)}[k]]

    def many(ref, count, sems, which):
        view = ref.at[pl.ds(0, count)]
        pltpu.make_async_copy(view, view, sems.at[which]).wait()

    def columns():
        many(side_p, 15, sp_sems, 1)
        many(side_l, 7, sl_sems, 1)
        side_rows[...] = jnp.zeros_like(side_rows)
        side_rows[0:16, :] = side_p[:, 0, :]
        side_rows[16:32, :] = side_p[:, 1, :]
        side_rows[32:40, :] = side_l[:, 0, :]
        side_rows[40:48, :] = side_l[:, 1, :]
        turned = side_rows[...].T
        lane = lax.broadcasted_iota(jnp.int32, (CHUNK, 128), 1)
        for s in range(16):
            place = pl.ds(s * CHUNK, CHUNK)
            wcol_p[place, :] = jnp.broadcast_to(turned[0:CHUNK, s : s + 1], (CHUNK, 128))
            tcol_p[place, :] = jnp.where(lane == 0, turned[0:CHUNK, 16 + s : 17 + s], 0.0)
        for s in range(8):
            place = pl.ds(s * CHUNK, CHUNK)
            wcol_l[place, :] = jnp.broadcast_to(turned[0:CHUNK, 32 + s : 33 + s], (CHUNK, 128))
            tcol_l[place, :] = jnp.where(lane == 0, turned[0:CHUNK, 40 + s : 41 + s], 0.0)

    def wide(n):
        return pl.ds(pl.multiple_of(n * WIDE, WIDE), WIDE)

    def batch(line, plane, middle):
        chunks = [(xl, hl, ol, il, q_l, wcol_l, tcol_l, slot) for slot in line]
        chunks += [(None, hp, op, ip, q_p, wcol_p, tcol_p, slot) for slot in plane]
        size = len(chunks) * CHUNK
        span = pl.ds(0, size)
        for k, chunk in enumerate(chunks):
            to, at_slot = pl.ds(k * CHUNK, CHUNK), rows(chunk[-1])
            if chunk[0] is None:
                xs[to, 0:512] = xpa[at_slot, :]
                xs[to, 512:1024] = xpb[at_slot, :]
            else:
                xs[to, :] = xl[c, at_slot, :]

        def put(which, lanes, value):
            for k, chunk in enumerate(chunks):
                piece = value[k * CHUNK : (k + 1) * CHUNK]
                if chunk[0] is None:
                    chunk[which][rows(chunk[-1]), lanes] = piece
                else:
                    chunk[which][c, rows(chunk[-1]), lanes] = piece

        for n in range(4):
            lanes = pl.ds(n * WIDE, WIDE)
            pre = dot(xs[span, :], w1[:, lanes])
            s = sigmoid(pre)
            value = (pre * s).astype(BF16)
            hs[span, lanes] = value
            put(1, lanes, value)
            slope[span, lanes] = s * (1.0 + pre * (1.0 - s))
        middle()
        for k, chunk in enumerate(chunks):
            to, at_slot = pl.ds(k * CHUNK, CHUNK), rows(chunk[-1])
            wcol[to, :] = chunk[5][at_slot, :]
        for n in range(4):
            lanes = pl.ds(n * WIDE, WIDE)
            pre = dot(hs[span, :], w2[:, lanes])
            s = sigmoid(pre)
            gain = gain_row[0:1, lanes]
            silu = pre * s * gain
            silu = silu[:, 0:128] + silu[:, 128:256]
            if n == 0:
                sig[span, :] = silu
            else:
                sig[span, :] += silu
            value = (twice(wcol[span, :]) * (s * (1.0 + pre * (1.0 - s))) * gain).astype(BF16)
            os[span, lanes] = value
            put(2, lanes, value)
        for n in range(4):
            lanes = pl.ds(n * WIDE, WIDE)
            back = dot_nt(os[span, :], w2[lanes, :])
            put(3, lanes, (back * slope[span, lanes]).astype(BF16))
        for k, chunk in enumerate(chunks):
            to, at_slot = pl.ds(k * CHUNK, CHUNK), rows(chunk[-1])
            chunk[4][at_slot, :] = sig[to, :] * wcol[to, :] - chunk[6][at_slot, :]
    sub = lax.broadcasted_iota(jnp.int32, (8, 128), 0)

    def packed(lines, first=0):
        value = jnp.zeros((8, 128), F32)
        for k, line in enumerate(lines):
            value = jnp.where(sub == first + k, line, value)
        return value

    partner = at(cc=1 - c)
    core_copies = []

    def share(view):
        k = len(core_copies)
        core_copies.append(send(view, view, core_send.at[k], core_recv.at[k], partner))

    def share_all(line):
        for slot in line:
            for ref in (xl, hl, ol, il):
                share(ref.at[c, rows(slot)])

    loads[7].wait()
    hop(1)
    loads[8].wait()
    line = line_slots(0) + line_slots(1)
    batch(line, plane_slots(0) + plane_slots(1), columns)
    for k in (2, 3):
        hop(k)
        share_all(line)
        line = line_slots(k)
        batch(line, plane_slots(k), lambda: None)
    share_all(line)

    def as_lines(ref, count):
        return [jnp.sum(ref[pl.ds(b * 128, 128), :].T, axis=0, keepdims=True) for b in range(count)]

    half_r[c] = packed(as_lines(q_l, 3), c * 3)
    share(half_r.at[c])
    r0p = packed(as_lines(q_p, 6))

    def gram(which):
        def block(n, carry):
            place = wide(n)
            one = dot_nt(xl[which, :, 0:512], xpa[place, :]) + dot_nt(xl[which, :, 512:1024], xpb[place, :])
            value = one * dot_nt(il[which], ip[place, :])
            value = value + dot_nt(hl[which], hp[place, :]) * dot_nt(ol[which], op[place, :])
            kern[which, :, place] = value
            return carry

        lax.fori_loop(0, 3, block, 0, unroll=3)

    gram(c)
    for copy in core_copies:
        copy.wait_recv()
    r0l = half_r[0] + half_r[1]
    gram(1 - c)

    def products(dp, dl):
        lines_l, sums = [], [None] * 6
        for b in range(6):
            part = kern.at[b // 3, pl.ds((b % 3) * 128, 128)]
            if dl is not None:
                col = jnp.broadcast_to(dl[b : b + 1, :], (128, 128)).T
            acc = None
            for t in range(6):
                tile = part[:, t * 128 : (t + 1) * 128]
                term = tile * dp[t : t + 1, :]
                acc = term if acc is None else acc + term
                if dl is not None:
                    down = jnp.sum((tile * col).reshape(16, 8, 128), axis=0)
                    sums[t] = down if sums[t] is None else sums[t] + down
            lines_l.append(jnp.sum(acc.T, axis=0, keepdims=True))
        lines_p = [jnp.sum(s, axis=0, keepdims=True) for s in sums] if dl is not None else []
        return lines_p, packed(lines_l)

    def start_plane(k, value):
        plane_buf[k, me_p] = value
        for peer in plane_peers:
            send(plane_buf.at[k, me_p], plane_buf.at[k, me_p], plane_sems.at[k, 0], plane_sems.at[k, 1], peer)

    def start_line(k, value):
        line_buf[k, me_l] = value
        for peer in line_peers:
            send(line_buf.at[k, me_l], line_buf.at[k, me_l], line_sems.at[k, 0], line_sems.at[k, 1], peer)

    def end_plane(k):
        many(plane_buf.at[k], 15, plane_sems.at[k], 1)
        return jnp.sum(plane_buf[k], axis=0)

    def end_line(k):
        many(line_buf.at[k], 15, line_sems.at[k], 1)
        return jnp.sum(line_buf[k], axis=0)

    def scalars(m, n):
        return [jnp.zeros((1, 128), F32)] * 6 + [jnp.broadcast_to(m, (1, 128)), jnp.broadcast_to(n, (1, 128))]

    lines_p, part_l = products(r0p, r0l)
    start_line(0, part_l)
    start_plane(0, packed(lines_p))
    mine = pl.ds(pl.multiple_of(z * 128, 128), 128)
    for b in range(6):
        place = pl.ds((b % 3) * 128, 128)
        x_t[:, b * 128 : (b + 1) * 128] = xl[b // 3, place, mine].astype(F32).T
        h_t[:, b * 128 : (b + 1) * 128] = hl[b // 3, place, mine].astype(F32).T
    w0p = end_plane(0) + DAMP * r0p
    w0l = end_line(0) + DAMP * r0l
    m0, m1 = total_of(r0l * r0l), total_of(r0l * w0l)
    lines_p, part_l = products(w0p, w0l)
    start_line(1, part_l)
    start_plane(1, packed(lines_p + scalars(m0, m1)[6:]))
    got = end_plane(1)
    u0p = got + DAMP * w0p
    u0l = end_line(1) + DAMP * w0l
    rr0, rw0 = got[6:7, :], got[7:8, :]
    al0 = rr0 / rw0
    r1l, w1l = r0l - al0 * w0l, w0l - al0 * u0l
    w1p = w0p - al0 * u0p
    m0, m1 = total_of(r1l * r1l), total_of(r1l * w1l)
    start_plane(2, packed(scalars(m0, m1)))
    _, part_l = products(w1p, None)
    start_line(2, part_l)
    basis = [
        jnp.concatenate([vector[b : b + 1, :] for b in range(6)], axis=1) for vector in (r0l, r1l, w1l, w0l)
    ]

    def summed(which, turned_ref, right):
        left = jnp.concatenate(
            [turned_ref[pl.ds(pl.multiple_of(c * 32 + 64 * k, 32), 32), :] for k in range(2)], axis=0
        )
        scaled = [left * across for across in basis]
        coarse = [value.astype(BF16) for value in scaled]
        fine = [(value - part.astype(F32)).astype(BF16) for value, part in zip(scaled, coarse)]
        stack = jnp.concatenate(coarse + fine, axis=0)
        for n in range(4):
            lanes = pl.ds(n * WIDE, WIDE)
            got = dot(stack, right[:, :, lanes].reshape(SET, WIDE))
            for k in range(4):
                terms[which, k, :, lanes] = got[64 * k : 64 * k + 64] + got[256 + 64 * k : 320 + 64 * k]

    summed(0, x_t, il)
    got = end_plane(2)
    u1l = end_line(2) + DAMP * w1l
    rr1, rw1 = got[6:7, :], got[7:8, :]
    be0 = rr1 / rr0
    al1 = rr1 / (rw1 - be0 * rr1 / al0)
    r2l = r1l - al1 * (w1l + be0 * w0l)
    w2l = w1l - al1 * (u1l + be0 * u0l)
    m0, m1 = total_of(r2l * r2l), total_of(r2l * w2l)
    start_plane(3, packed(scalars(m0, m1)))
    summed(1, h_t, ol)
    got = end_plane(3)
    rr2, rw2 = got[6:7, :], got[7:8, :]
    be1 = rr2 / rr1
    al2 = rr2 / (rw2 - be1 * rr2 / al1)
    def combined(which, factors):
        value = None
        for k, factor in enumerate(factors):
            term = terms[which, k] * jnp.concatenate([-LEARN * factor] * 8, axis=1)
            value = term if value is None else value + term
        return value

    both = al1 + al2 * be1
    one = combined(0, (al0 + both * be0, both + al2, -al2 * al1, -al2 * al1 * be0))
    two = combined(1, (al0 + both * be0, both + al2, -al2 * al1, -al2 * al1 * be0))
    sub_wide = lax.broadcasted_iota(jnp.int32, (8, 1024), 0)
    for e in range(8):
        f, s = one[8 * e : 8 * e + 8], two[8 * e : 8 * e + 8]
        out_send[2 * e] = jnp.where(sub_wide < 4, f, pltpu.roll(s, 4, 0)).astype(BF16)
        out_send[2 * e + 1] = jnp.where(sub_wide < 4, pltpu.roll(f, 4, 0), s).astype(BF16)
    for k, peer in zip(plane_order, plane_peers):
        dest = lax.rem(y + k // 4, 4) * 4 + lax.rem(x + k % 4, 4)
        send(out_send.at[dest], out_recv.at[me_p], out_sems.at[0], out_sems.at[1], peer)
    out_recv[me_p] = out_send[me_p]
    many(out_recv, 15, out_sems, 1)
    result = jnp.sum(out_recv[...].astype(F32), axis=0)
    out_ref[:, 0:1024] = result[0:4]
    out_ref[:, 1024:2048] = result[4:8]

    for copy in pending + core_copies:
        copy.wait_send()
    many(side_p, 15, sp_sems, 0)
    many(side_l, 7, sl_sems, 0)
    for k in range(4):
        many(plane_buf.at[k], 15, plane_sems.at[k], 0)
    for k in range(3):
        many(line_buf.at[k], 15, line_sems.at[k], 0)
    many(out_send, 15, out_sems, 0)


def shards(inputs, first_weight, second_weight, readout, target, counts, views):
    vmem = pl.BlockSpec(memory_space=pltpu.VMEM)
    hbm = pl.BlockSpec(memory_space=pltpu.HBM)
    dma = pltpu.SemaphoreType.DMA
    return pl.pallas_call(
        step_kernel,
        out_shape=jax.ShapeDtypeStruct((4, 2048), F32),
        in_specs=[hbm] * 7,
        out_specs=vmem,
        scratch_shapes=[
            pltpu.VMEM((8, 128), BF16), pltpu.VMEM((1, CHUNK), F32),
            pltpu.VMEM((1, CHUNK), jnp.int32), pltpu.VMEM((1, CHUNK), jnp.int32),
            pltpu.VMEM((1, 1024), F32), pltpu.VMEM((2, 128), F32),
            pltpu.VMEM((1024, 1024), BF16), pltpu.VMEM((1024, 1024), BF16),
            pltpu.VMEM((SET, 512), BF16), pltpu.VMEM((SET, 512), BF16),
            pltpu.VMEM((SET, 1024), BF16), pltpu.VMEM((SET, 1024), BF16), pltpu.VMEM((SET, 1024), BF16),
            pltpu.VMEM((2, HALF, 1024), BF16), pltpu.VMEM((2, HALF, 1024), BF16),
            pltpu.VMEM((2, HALF, 1024), BF16), pltpu.VMEM((2, HALF, 1024), BF16),
            pltpu.VMEM((HALF, 1024), BF16), pltpu.VMEM((HALF, 1024), BF16), pltpu.VMEM((HALF, 1024), BF16),
            pltpu.VMEM((HALF, 1024), F32), pltpu.VMEM((HALF, 128), F32),
            pltpu.VMEM((2, HALF, SET), F32),
            pltpu.VMEM((16, 2, 128), F32), pltpu.VMEM((8, 2, 128), F32), pltpu.VMEM((128, 128), F32),
            pltpu.VMEM((SET, 128), F32), pltpu.VMEM((SET, 128), F32),
            pltpu.VMEM((HALF, 128), F32), pltpu.VMEM((HALF, 128), F32), pltpu.VMEM((HALF, 128), F32),
            pltpu.VMEM((SET, 128), F32), pltpu.VMEM((HALF, 128), F32),
            pltpu.VMEM((2, 8, 128), F32), pltpu.VMEM((128, SET), F32), pltpu.VMEM((128, SET), F32),
            pltpu.VMEM((2, 4, 64, 1024), F32), pltpu.VMEM((4, 16, 8, 128), F32), pltpu.VMEM((3, 16, 8, 128), F32),
            pltpu.VMEM((16, 8, 1024), BF16), pltpu.VMEM((16, 8, 1024), BF16),
            dma((9,)), dma((16,)), dma((16,)), dma((16,)), dma((16,)), dma((16,)), dma((16,)),
            dma((33,)), dma((33,)), dma((2,)), dma((2,)), dma((4, 2)), dma((3, 2)), dma((2,)),
        ],
        compiler_params=pltpu.CompilerParams(
            collective_id=0, has_side_effects=True, vmem_limit_bytes=56 * 1024 * 1024
        ),
    )(
        inputs, first_weight, second_weight, readout.reshape(8, 128),
        target.reshape(1, CHUNK), counts.reshape(1, CHUNK), views.reshape(1, CHUNK),
    )


def solution(mesh):
    split = Mesh(mesh.devices.reshape(8, 2, 2, 2, 4), AXES)
    return jax.shard_map(
        shards,
        mesh=split,
        in_specs=(P(AXES, None), P(), P(), P(), P(AXES), P(AXES), P(AXES)),
        out_specs=P(AXES, None),
        check_vma=False,
    )
```

```python
import functools

import jax
import jax.numpy as jnp
from jax import lax
from jax.experimental import pallas as pl
from jax.experimental.pallas import tpu as pltpu
from jax.sharding import Mesh
from jax.sharding import PartitionSpec as P

VIEWS = 2000
DAMP = 4.0
LEARN = 8.0
AXES = ("z", "yh", "core", "yl", "x")
MESH = pl.DeviceIdType.MESH
F32 = jnp.float32
BF16 = jnp.bfloat16
CHUNK = 48
HALF = 384
SET = 768
WIDE = 256
NT = (((1,), (1,)), ((), ()))


def dot(a, b):
    return jnp.dot(a, b, preferred_element_type=F32)


def dot_nt(a, b):
    return lax.dot_general(a, b, NT, preferred_element_type=F32)


def sigmoid(value):
    return 0.5 * jnp.tanh(0.5 * value) + 0.5


def twice(column):
    return jnp.concatenate([column, column], axis=1)


def total_of(value):
    return jnp.sum(jnp.sum(value, axis=1, keepdims=True), axis=0, keepdims=True)


def step_kernel(
    x_hbm, w1_hbm, w2_hbm, gain_hbm, target_hbm, counts_hbm, views_hbm, out_ref,
    gain_in, target_in, counts_in, views_in, gain_row, side_ref,
    w1, w2, xpa, xpb, hp, op, ip, xl, hl, ol, il, xs, hs, os, slope, wcol, kern,
    side_p, side_l, side_rows, wcol_p, tcol_p, wcol_l, tcol_l, sig, q_p, q_l,
    half_r, x_t, h_t, terms, plane_buf, line_buf, out_send, out_recv,
    load_sem, a_send, a_recv, b_send, b_recv, z_send, z_recv,
    core_send, core_recv, sp_sems, sl_sems, plane_sems, line_sems, out_sems,
):
    z, yh, c, yl, x = (lax.axis_index(name) for name in AXES)
    y = yh * 2 + yl
    me_p = y * 4 + x
    me_l = c * 8 + z

    def at(xx=None, yy=None, zz=None, cc=None):
        xx = x if xx is None else lax.rem(xx, 4)
        yy = y if yy is None else lax.rem(yy, 4)
        zz = z if zz is None else lax.rem(zz, 8)
        cc = c if cc is None else cc
        return (zz, yy // 2, cc, lax.rem(yy, 2), xx)

    plane_order = (10, 6, 14, 9, 11, 2, 8, 5, 7, 13, 15, 1, 3, 4, 12)
    line_order = (4, 3, 5, 2, 6, 1, 7)
    plane_peers = [at(xx=x + k % 4, yy=y + k // 4) for k in plane_order]
    line_same = [at(zz=z + k) for k in line_order]
    line_peers = [at(zz=z + k, cc=c if q == 0 else 1 - c) for k in line_order for q in range(2)] + [at(cc=1 - c)]

    def send(src, dst, ssem, rsem, dev):
        copy = pltpu.make_async_remote_copy(
            src_ref=src, dst_ref=dst, send_sem=ssem, recv_sem=rsem,
            device_id=dev, device_id_type=MESH,
        )
        copy.start()
        return copy

    def rows(slot, count=1):
        return pl.ds(pl.multiple_of(slot * CHUNK, CHUNK), count * CHUNK)

    loads = [
        pltpu.make_async_copy(x_hbm.at[:, pl.ds(0, 512)], xpa.at[rows(me_p)], load_sem.at[0]),
        pltpu.make_async_copy(x_hbm.at[:, pl.ds(512, 512)], xpb.at[rows(me_p)], load_sem.at[1]),
        pltpu.make_async_copy(x_hbm, xl.at[c, rows(z)], load_sem.at[2]),
        pltpu.make_async_copy(counts_hbm, counts_in, load_sem.at[3]),
        pltpu.make_async_copy(views_hbm, views_in, load_sem.at[4]),
        pltpu.make_async_copy(target_hbm, target_in, load_sem.at[5]),
        pltpu.make_async_copy(gain_hbm, gain_in, load_sem.at[6]),
        pltpu.make_async_copy(w1_hbm, w1, load_sem.at[7]),
        pltpu.make_async_copy(w2_hbm, w2, load_sem.at[8]),
    ]
    for load in loads:
        load.start()

    barrier = pltpu.get_barrier_semaphore()
    for peer in plane_peers + line_peers:
        pl.semaphore_signal(barrier, inc=1, device_id=peer, device_id_type=MESH)
    for load in loads[:7]:
        load.wait()
    side_ref[...] = jnp.zeros_like(side_ref)
    angle = (2.0 * jnp.pi / VIEWS) * views_in[...].astype(F32)
    side_ref[0:1, 0:CHUNK] = counts_in[...].astype(F32) / 16.0 * (1.0 + 0.5 * jnp.cos(angle))
    side_ref[1:2, 0:CHUNK] = target_in[...]
    gain = gain_in[...].astype(F32)
    for k in range(8):
        gain_row[:, k * 128 : (k + 1) * 128] = gain[k : k + 1, :]
    pl.semaphore_wait(barrier, 30)

    xn, xq = at(xx=x + 1), at(xx=x + 3)
    yn, yq = at(yy=y + 1), at(yy=y + 3)
    zn, zq = at(zz=z + 1), at(zz=z + 7)
    pending = []

    def go(ref, index, ssem, rsem, k, dev):
        copy = send(ref.at[index], ref.at[index], ssem.at[k], rsem.at[k], dev)
        pending.append(copy)
        return copy

    low, high = pl.ds(0, 256), pl.ds(256, 256)
    offsets = (0, 3, 1, 2)

    class Spread:
        def __init__(self, ref, place, near, far, ssem, rsem):
            self.ref, self.place, self.near, self.far = ref, place, near, far
            self.sems, self.sent = (ssem, rsem), {}

        def go(self, k, d1, d2, dev, lanes=None):
            index = (rows(self.place(d1, d2)),) + (() if lanes is None else (lanes,))
            self.sent[k] = go(self.ref, index, *self.sems, k, dev)

        def arrived(self, *keys):
            for k in keys:
                self.sent[k].wait_recv()

        def second(self, j):
            for side in range(2):
                self.go(4 + 4 * side + j, offsets[j], 0, self.far[side])

        def start(self):
            self.go(0, 0, 0, self.near[0])
            self.go(1, 0, 0, self.near[1])
            self.second(0)

        def hop(self, k):
            if k == 1:
                self.arrived(0)
                self.go(2, 3, 0, self.near[0], low)
                self.arrived(1)
                self.go(3, 1, 0, self.near[1], high)
                self.second(1)
                self.second(2)
                self.arrived(4, 8)
                self.go(12, 0, 3, self.far[0])
            elif k == 2:
                self.arrived(2, 3)
                self.second(3)
                self.go(15, 2, 0, self.far[2])
                self.arrived(5, 9)
                self.go(13, 3, 1, self.far[1])
                self.arrived(6, 10)
                self.go(14, 1, 1, self.far[1])
                self.arrived(12)
            else:
                self.arrived(7, 11, 13, 14, 15)

    half_a = Spread(
        xpa, lambda d1, d2: lax.rem(y + d2, 4) * 4 + lax.rem(x + d1, 4), (xn, xq), (yn, yq, at(yy=y + 2)), a_send, a_recv
    )
    half_b = Spread(
        xpb, lambda d1, d2: lax.rem(y + d1, 4) * 4 + lax.rem(x + d2, 4), (yn, yq), (xn, xq, at(xx=x + 2)), b_send, b_recv
    )
    ring_sent = {}
    parts = (pl.ds(0, 512), pl.ds(512, 512))

    def ring(step, side, h, dist, dev):
        owner = lax.rem(z + (8 - dist if side == 0 else dist), 8)
        key = step * 4 + side * 2 + h
        ring_sent[key] = go(xl, (c, rows(owner), parts[h]), z_send, z_recv, key, dev)

    def ring_hop(k, h):
        for side in range(2):
            ring_sent[(k - 1) * 4 + side * 2 + h].wait_recv()
            if k < 3:
                ring(k, side, h, k, (zn, zq)[side])
            if k == 2 and side == h:
                ring(3, side, h, k, (at(zz=z + 2), at(zz=z + 6))[side])
        if k == 3 and h == 1:
            for key in (12, 15):
                ring_sent[key].wait_recv()

    half_a.start()
    half_b.start()
    for h in range(2):
        for side in range(2):
            ring(0, side, h, 0, (zn, zq)[side])
    for k in range(15):
        send(side_ref, side_p.at[me_p], sp_sems.at[0], sp_sems.at[1], plane_peers[k])
    for k in range(7):
        send(side_ref, side_l.at[z], sl_sems.at[0], sl_sems.at[1], line_same[k])
    side_p[me_p] = side_ref[...]
    side_l[z] = side_ref[...]

    def hop(k):
        ring_hop(k, 0)
        half_a.hop(k)
        ring_hop(k, 1)
        half_b.hop(k)

    near = {0: ((0, 0),), 1: ((0, 1), (0, 3), (1, 0), (3, 0)),
            2: ((2, 0), (0, 2), (1, 1), (1, 3), (3, 1), (3, 3)),
            3: ((2, 1), (2, 3), (1, 2), (3, 2), (2, 2))}

    def plane_slots(k):
        return [lax.rem(y + dy, 4) * 4 + lax.rem(x + dx, 4) for dx, dy in near[k]]

    def line_slots(k):
        return [lax.rem(z + d, 8) for d in {0: (0,), 1: (1, 7), 2: (2, 6), 3: (3, 5, 4)}[k]]

    def many(ref, count, sems, which):
        view = ref.at[pl.ds(0, count)]
        pltpu.make_async_copy(view, view, sems.at[which]).wait()

    def columns():
        many(side_p, 15, sp_sems, 1)
        many(side_l, 7, sl_sems, 1)
        side_rows[...] = jnp.zeros_like(side_rows)
        side_rows[0:16, :] = side_p[:, 0, :]
        side_rows[16:32, :] = side_p[:, 1, :]
        side_rows[32:40, :] = side_l[:, 0, :]
        side_rows[40:48, :] = side_l[:, 1, :]
        turned = side_rows[...].T
        lane = lax.broadcasted_iota(jnp.int32, (CHUNK, 128), 1)
        for s in range(16):
            place = pl.ds(s * CHUNK, CHUNK)
            wcol_p[place, :] = jnp.broadcast_to(turned[0:CHUNK, s : s + 1], (CHUNK, 128))
            tcol_p[place, :] = jnp.where(lane == 0, turned[0:CHUNK, 16 + s : 17 + s], 0.0)
        for s in range(8):
            place = pl.ds(s * CHUNK, CHUNK)
            wcol_l[place, :] = jnp.broadcast_to(turned[0:CHUNK, 32 + s : 33 + s], (CHUNK, 128))
            tcol_l[place, :] = jnp.where(lane == 0, turned[0:CHUNK, 40 + s : 41 + s], 0.0)

    def wide(n):
        return pl.ds(pl.multiple_of(n * WIDE, WIDE), WIDE)

    def batch(line, plane, middle):
        chunks = [(xl, hl, ol, il, q_l, wcol_l, tcol_l, slot) for slot in line]
        chunks += [(None, hp, op, ip, q_p, wcol_p, tcol_p, slot) for slot in plane]
        size = len(chunks) * CHUNK
        span = pl.ds(0, size)
        for k, chunk in enumerate(chunks):
            to, at_slot = pl.ds(k * CHUNK, CHUNK), rows(chunk[-1])
            if chunk[0] is None:
                xs[to, 0:512] = xpa[at_slot, :]
                xs[to, 512:1024] = xpb[at_slot, :]
            else:
                xs[to, :] = xl[c, at_slot, :]

        def put(which, lanes, value):
            for k, chunk in enumerate(chunks):
                piece = value[k * CHUNK : (k + 1) * CHUNK]
                if chunk[0] is None:
                    chunk[which][rows(chunk[-1]), lanes] = piece
                else:
                    chunk[which][c, rows(chunk[-1]), lanes] = piece

        for n in range(4):
            lanes = pl.ds(n * WIDE, WIDE)
            pre = dot(xs[span, :], w1[:, lanes])
            s = sigmoid(pre)
            value = (pre * s).astype(BF16)
            hs[span, lanes] = value
            put(1, lanes, value)
            slope[span, lanes] = s * (1.0 + pre * (1.0 - s))
        middle()
        for k, chunk in enumerate(chunks):
            to, at_slot = pl.ds(k * CHUNK, CHUNK), rows(chunk[-1])
            wcol[to, :] = chunk[5][at_slot, :]
        for n in range(4):
            lanes = pl.ds(n * WIDE, WIDE)
            pre = dot(hs[span, :], w2[:, lanes])
            s = sigmoid(pre)
            gain = gain_row[0:1, lanes]
            silu = pre * s * gain
            silu = silu[:, 0:128] + silu[:, 128:256]
            if n == 0:
                sig[span, :] = silu
            else:
                sig[span, :] += silu
            value = (twice(wcol[span, :]) * (s * (1.0 + pre * (1.0 - s))) * gain).astype(BF16)
            os[span, lanes] = value
            put(2, lanes, value)
        for n in range(4):
            lanes = pl.ds(n * WIDE, WIDE)
            back = dot_nt(os[span, :], w2[lanes, :])
            put(3, lanes, (back * slope[span, lanes]).astype(BF16))
        for k, chunk in enumerate(chunks):
            to, at_slot = pl.ds(k * CHUNK, CHUNK), rows(chunk[-1])
            chunk[4][at_slot, :] = sig[to, :] * wcol[to, :] - chunk[6][at_slot, :]
    sub = lax.broadcasted_iota(jnp.int32, (8, 128), 0)

    def packed(lines, first=0):
        value = jnp.zeros((8, 128), F32)
        for k, line in enumerate(lines):
            value = jnp.where(sub == first + k, line, value)
        return value

    partner = at(cc=1 - c)
    core_copies = []

    def share(view):
        k = len(core_copies)
        core_copies.append(send(view, view, core_send.at[k], core_recv.at[k], partner))

    def share_all(line):
        for slot in line:
            for ref in (xl, hl, ol, il):
                share(ref.at[c, rows(slot)])

    loads[7].wait()
    hop(1)
    loads[8].wait()
    line = line_slots(0) + line_slots(1)
    batch(line, plane_slots(0) + plane_slots(1), columns)
    for k in (2, 3):
        hop(k)
        share_all(line)
        line = line_slots(k)
        batch(line, plane_slots(k), lambda: None)
    share_all(line)

    def as_lines(ref, count):
        return [jnp.sum(ref[pl.ds(b * 128, 128), :].T, axis=0, keepdims=True) for b in range(count)]

    half_r[c] = packed(as_lines(q_l, 3), c * 3)
    share(half_r.at[c])
    r0p = packed(as_lines(q_p, 6))

    def gram(which):
        def block(n, carry):
            place = wide(n)
            one = dot_nt(xl[which, :, 0:512], xpa[place, :]) + dot_nt(xl[which, :, 512:1024], xpb[place, :])
            value = one * dot_nt(il[which], ip[place, :])
            value = value + dot_nt(hl[which], hp[place, :]) * dot_nt(ol[which], op[place, :])
            kern[which, :, place] = value
            return carry

        lax.fori_loop(0, 3, block, 0, unroll=3)

    gram(c)
    for copy in core_copies:
        copy.wait_recv()
    r0l = half_r[0] + half_r[1]
    gram(1 - c)

    def products(dp, dl):
        lines_l, sums = [], [None] * 6
        for b in range(6):
            part = kern.at[b // 3, pl.ds((b % 3) * 128, 128)]
            if dl is not None:
                col = jnp.broadcast_to(dl[b : b + 1, :], (128, 128)).T
            acc = None
            for t in range(6):
                tile = part[:, t * 128 : (t + 1) * 128]
                term = tile * dp[t : t + 1, :]
                acc = term if acc is None else acc + term
                if dl is not None:
                    down = jnp.sum((tile * col).reshape(16, 8, 128), axis=0)
                    sums[t] = down if sums[t] is None else sums[t] + down
            lines_l.append(jnp.sum(acc.T, axis=0, keepdims=True))
        lines_p = [jnp.sum(s, axis=0, keepdims=True) for s in sums] if dl is not None else []
        return lines_p, packed(lines_l)

    def start_plane(k, value):
        plane_buf[k, me_p] = value
        for peer in plane_peers:
            send(plane_buf.at[k, me_p], plane_buf.at[k, me_p], plane_sems.at[k, 0], plane_sems.at[k, 1], peer)

    def start_line(k, value):
        line_buf[k, me_l] = value
        for peer in line_peers:
            send(line_buf.at[k, me_l], line_buf.at[k, me_l], line_sems.at[k, 0], line_sems.at[k, 1], peer)

    def end_plane(k):
        many(plane_buf.at[k], 15, plane_sems.at[k], 1)
        return jnp.sum(plane_buf[k], axis=0)

    def end_line(k):
        many(line_buf.at[k], 15, line_sems.at[k], 1)
        return jnp.sum(line_buf[k], axis=0)

    def scalars(m, n):
        return [jnp.zeros((1, 128), F32)] * 6 + [jnp.broadcast_to(m, (1, 128)), jnp.broadcast_to(n, (1, 128))]

    def summed(which, at_term, vectors):
        turned_ref, right = ((x_t, il), (h_t, ol))[which]
        left = jnp.concatenate(
            [turned_ref[pl.ds(pl.multiple_of(c * 32 + 64 * k, 32), 32), :] for k in range(2)], axis=0
        )
        basis = [jnp.concatenate([vector[b : b + 1, :] for b in range(6)], axis=1) for vector in vectors]
        scaled = [left * across for across in basis]
        coarse = [value.astype(BF16) for value in scaled]
        fine = [(value - part.astype(F32)).astype(BF16) for value, part in zip(scaled, coarse)]
        stack = jnp.concatenate(coarse + fine, axis=0)
        half = 64 * len(vectors)
        for n in range(4):
            lanes = pl.ds(n * WIDE, WIDE)
            found = dot(stack, right[:, :, lanes].reshape(SET, WIDE))
            for k in range(len(vectors)):
                near, far = found[64 * k : 64 * k + 64], found[half + 64 * k : half + 64 * k + 64]
                terms[which, at_term + k, :, lanes] = near + far

    sub_wide = lax.broadcasted_iota(jnp.int32, (8, 1024), 0)

    def stage(slot, one, two):
        for e in range(8):
            f, s = one[8 * e : 8 * e + 8], two[8 * e : 8 * e + 8]
            out_send[slot, 2 * e] = jnp.where(sub_wide < 4, f, pltpu.roll(s, 4, 0)).astype(BF16)
            out_send[slot, 2 * e + 1] = jnp.where(sub_wide < 4, pltpu.roll(f, 4, 0), s).astype(BF16)
        out_recv[slot, me_p] = out_send[slot, me_p]

    def give(slot):
        for k, peer in zip(plane_order, plane_peers):
            dest = lax.rem(y + k // 4, 4) * 4 + lax.rem(x + k % 4, 4)
            send(out_send.at[slot, dest], out_recv.at[slot, me_p], out_sems.at[slot, 0], out_sems.at[slot, 1], peer)

    def whole(factor):
        return jnp.concatenate([factor] * 8, axis=1)

    lines_p, part_l = products(r0p, r0l)
    start_line(0, part_l)
    start_plane(0, packed(lines_p))
    mine = pl.ds(pl.multiple_of(z * 128, 128), 128)
    for b in range(6):
        place = pl.ds((b % 3) * 128, 128)
        x_t[:, b * 128 : (b + 1) * 128] = xl[b // 3, place, mine].astype(F32).T
        h_t[:, b * 128 : (b + 1) * 128] = hl[b // 3, place, mine].astype(F32).T
    summed(0, 0, (r0l,))
    summed(1, 0, (r0l,))
    stage(0, terms[0, 0], terms[1, 0])
    w0p = end_plane(0) + DAMP * r0p
    w0l = end_line(0) + DAMP * r0l
    m0, m1 = total_of(r0l * r0l), total_of(r0l * w0l)
    lines_p, part_l = products(w0p, w0l)
    start_line(1, part_l)
    start_plane(1, packed(lines_p + scalars(m0, m1)[6:]))
    give(0)
    got = end_plane(1)
    u0p = got + DAMP * w0p
    u0l = end_line(1) + DAMP * w0l
    rr0, rw0 = got[6:7, :], got[7:8, :]
    al0 = rr0 / rw0
    r1l, w1l = r0l - al0 * w0l, w0l - al0 * u0l
    w1p = w0p - al0 * u0p
    m0, m1 = total_of(r1l * r1l), total_of(r1l * w1l)
    start_plane(2, packed(scalars(m0, m1)))
    _, part_l = products(w1p, None)
    start_line(2, part_l)
    summed(0, 1, (r1l, w1l, w0l))
    summed(1, 1, (r1l, w1l, w0l))
    stage(1, terms[0, 1], terms[1, 1])
    give(1)
    got = end_plane(2)
    u1l = end_line(2) + DAMP * w1l
    rr1, rw1 = got[6:7, :], got[7:8, :]
    be0 = rr1 / rr0
    al1 = rr1 / (rw1 - be0 * rr1 / al0)
    r2l = r1l - al1 * (w1l + be0 * w0l)
    w2l = w1l - al1 * (u1l + be0 * u0l)
    m0, m1 = total_of(r2l * r2l), total_of(r2l * w2l)
    start_plane(3, packed(scalars(m0, m1)))
    stage(2, *[
        terms[k, 1] - whole(al1) * (terms[k, 2] + whole(be0) * terms[k, 3]) for k in range(2)
    ])
    give(2)
    got = end_plane(3)
    rr2, rw2 = got[6:7, :], got[7:8, :]
    be1 = rr2 / rr1
    al2 = rr2 / (rw2 - be1 * rr2 / al1)
    both = al1 + al2 * be1
    result = None
    for slot, factor in enumerate((al0 + both * be0, both, al2)):
        many(out_recv.at[slot], 15, out_sems.at[slot], 1)
        term = jnp.sum(out_recv[slot].astype(F32), axis=0) * whole(-LEARN * factor)
        result = term if result is None else result + term
    out_ref[:, 0:1024] = result[0:4]
    out_ref[:, 1024:2048] = result[4:8]

    for copy in pending + core_copies:
        copy.wait_send()
    many(side_p, 15, sp_sems, 0)
    many(side_l, 7, sl_sems, 0)
    for k in range(4):
        many(plane_buf.at[k], 15, plane_sems.at[k], 0)
    for k in range(3):
        many(line_buf.at[k], 15, line_sems.at[k], 0)
    for slot in range(3):
        many(out_send.at[slot], 15, out_sems.at[slot], 0)


def shards(inputs, first_weight, second_weight, readout, target, counts, views):
    vmem = pl.BlockSpec(memory_space=pltpu.VMEM)
    hbm = pl.BlockSpec(memory_space=pltpu.HBM)
    dma = pltpu.SemaphoreType.DMA
    return pl.pallas_call(
        step_kernel,
        out_shape=jax.ShapeDtypeStruct((4, 2048), F32),
        in_specs=[hbm] * 7,
        out_specs=vmem,
        scratch_shapes=[
            pltpu.VMEM((8, 128), BF16), pltpu.VMEM((1, CHUNK), F32),
            pltpu.VMEM((1, CHUNK), jnp.int32), pltpu.VMEM((1, CHUNK), jnp.int32),
            pltpu.VMEM((1, 1024), F32), pltpu.VMEM((2, 128), F32),
            pltpu.VMEM((1024, 1024), BF16), pltpu.VMEM((1024, 1024), BF16),
            pltpu.VMEM((SET, 512), BF16), pltpu.VMEM((SET, 512), BF16),
            pltpu.VMEM((SET, 1024), BF16), pltpu.VMEM((SET, 1024), BF16), pltpu.VMEM((SET, 1024), BF16),
            pltpu.VMEM((2, HALF, 1024), BF16), pltpu.VMEM((2, HALF, 1024), BF16),
            pltpu.VMEM((2, HALF, 1024), BF16), pltpu.VMEM((2, HALF, 1024), BF16),
            pltpu.VMEM((HALF, 1024), BF16), pltpu.VMEM((HALF, 1024), BF16), pltpu.VMEM((HALF, 1024), BF16),
            pltpu.VMEM((HALF, 1024), F32), pltpu.VMEM((HALF, 128), F32),
            pltpu.VMEM((2, HALF, SET), F32),
            pltpu.VMEM((16, 2, 128), F32), pltpu.VMEM((8, 2, 128), F32), pltpu.VMEM((128, 128), F32),
            pltpu.VMEM((SET, 128), F32), pltpu.VMEM((SET, 128), F32),
            pltpu.VMEM((HALF, 128), F32), pltpu.VMEM((HALF, 128), F32), pltpu.VMEM((HALF, 128), F32),
            pltpu.VMEM((SET, 128), F32), pltpu.VMEM((HALF, 128), F32),
            pltpu.VMEM((2, 8, 128), F32), pltpu.VMEM((128, SET), F32), pltpu.VMEM((128, SET), F32),
            pltpu.VMEM((2, 4, 64, 1024), F32), pltpu.VMEM((4, 16, 8, 128), F32), pltpu.VMEM((3, 16, 8, 128), F32),
            pltpu.VMEM((3, 16, 8, 1024), BF16), pltpu.VMEM((3, 16, 8, 1024), BF16),
            dma((9,)), dma((16,)), dma((16,)), dma((16,)), dma((16,)), dma((16,)), dma((16,)),
            dma((33,)), dma((33,)), dma((2,)), dma((2,)), dma((4, 2)), dma((3, 2)), dma((3, 2)),
        ],
        compiler_params=pltpu.CompilerParams(
            collective_id=0, has_side_effects=True, vmem_limit_bytes=56 * 1024 * 1024
        ),
    )(
        inputs, first_weight, second_weight, readout.reshape(8, 128),
        target.reshape(1, CHUNK), counts.reshape(1, CHUNK), views.reshape(1, CHUNK),
    )


def solution(mesh):
    split = Mesh(mesh.devices.reshape(8, 2, 2, 2, 4), AXES)
    return jax.shard_map(
        shards,
        mesh=split,
        in_specs=(P(AXES, None), P(), P(), P(), P(AXES), P(AXES), P(AXES)),
        out_specs=P(AXES, None),
        check_vma=False,
    )
```

```python
import functools

import jax
import jax.numpy as jnp
from jax import lax
from jax.experimental import pallas as pl
from jax.experimental.pallas import tpu as pltpu
from jax.sharding import Mesh
from jax.sharding import PartitionSpec as P

VIEWS = 2000
DAMP = 4.0
LEARN = 8.0
AXES = ("z", "yh", "core", "yl", "x")
MESH = pl.DeviceIdType.MESH
F32 = jnp.float32
BF16 = jnp.bfloat16
CHUNK = 48
HALF = 384
SET = 768
WIDE = 256
NT = (((1,), (1,)), ((), ()))


def dot(a, b):
    return jnp.dot(a, b, preferred_element_type=F32)


def dot_nt(a, b):
    return lax.dot_general(a, b, NT, preferred_element_type=F32)


def sigmoid(value):
    return 0.5 * jnp.tanh(0.5 * value) + 0.5


def twice(column):
    return jnp.concatenate([column, column], axis=1)


def total_of(value):
    return jnp.sum(jnp.sum(value, axis=1, keepdims=True), axis=0, keepdims=True)


def step_kernel(
    x_hbm, w1_hbm, w2_hbm, gain_hbm, target_hbm, counts_hbm, views_hbm, out_ref,
    gain_in, target_in, counts_in, views_in, gain_row, side_ref,
    w1, w2, xpa, xpb, hp, op, ip, xl, hl, ol, il, xs, hs, os, slope, wcol, kern,
    side_p, side_l, side_rows, wcol_p, tcol_p, wcol_l, tcol_l, sig, q_p, q_l,
    half_r, x_t, h_t, terms, plane_buf, line_buf, out_send, out_recv,
    load_sem, a_send, a_recv, b_send, b_recv, z_send, z_recv,
    core_send, core_recv, sp_sems, sl_sems, plane_sems, line_sems, out_sems,
):
    z, yh, c, yl, x = (lax.axis_index(name) for name in AXES)
    y = yh * 2 + yl
    me_p = y * 4 + x
    me_l = c * 8 + z

    def at(xx=None, yy=None, zz=None, cc=None):
        xx = x if xx is None else lax.rem(xx, 4)
        yy = y if yy is None else lax.rem(yy, 4)
        zz = z if zz is None else lax.rem(zz, 8)
        cc = c if cc is None else cc
        return (zz, yy // 2, cc, lax.rem(yy, 2), xx)

    plane_order = (10, 6, 14, 9, 11, 2, 8, 5, 7, 13, 15, 1, 3, 4, 12)
    line_order = (4, 3, 5, 2, 6, 1, 7)
    plane_peers = [at(xx=x + k % 4, yy=y + k // 4) for k in plane_order]
    line_same = [at(zz=z + k) for k in line_order]
    line_peers = [at(zz=z + k, cc=c if q == 0 else 1 - c) for k in line_order for q in range(2)] + [at(cc=1 - c)]

    def send(src, dst, ssem, rsem, dev):
        copy = pltpu.make_async_remote_copy(
            src_ref=src, dst_ref=dst, send_sem=ssem, recv_sem=rsem,
            device_id=dev, device_id_type=MESH,
        )
        copy.start()
        return copy

    def rows(slot, count=1):
        return pl.ds(pl.multiple_of(slot * CHUNK, CHUNK), count * CHUNK)

    loads = [
        pltpu.make_async_copy(x_hbm.at[:, pl.ds(0, 512)], xpa.at[rows(me_p)], load_sem.at[0]),
        pltpu.make_async_copy(x_hbm.at[:, pl.ds(512, 512)], xpb.at[rows(me_p)], load_sem.at[1]),
        pltpu.make_async_copy(x_hbm, xl.at[c, rows(z)], load_sem.at[2]),
        pltpu.make_async_copy(counts_hbm, counts_in, load_sem.at[3]),
        pltpu.make_async_copy(views_hbm, views_in, load_sem.at[4]),
        pltpu.make_async_copy(target_hbm, target_in, load_sem.at[5]),
        pltpu.make_async_copy(gain_hbm, gain_in, load_sem.at[6]),
        pltpu.make_async_copy(w1_hbm, w1, load_sem.at[7]),
        pltpu.make_async_copy(w2_hbm, w2, load_sem.at[8]),
    ]
    for load in loads:
        load.start()

    barrier = pltpu.get_barrier_semaphore()
    for peer in plane_peers + line_peers:
        pl.semaphore_signal(barrier, inc=1, device_id=peer, device_id_type=MESH)
    for load in loads[:7]:
        load.wait()
    side_ref[...] = jnp.zeros_like(side_ref)
    angle = (2.0 * jnp.pi / VIEWS) * views_in[...].astype(F32)
    side_ref[0:1, 0:CHUNK] = counts_in[...].astype(F32) / 16.0 * (1.0 + 0.5 * jnp.cos(angle))
    side_ref[1:2, 0:CHUNK] = target_in[...]
    gain = gain_in[...].astype(F32)
    for k in range(8):
        gain_row[:, k * 128 : (k + 1) * 128] = gain[k : k + 1, :]
    pl.semaphore_wait(barrier, 30)

    xn, xq = at(xx=x + 1), at(xx=x + 3)
    yn, yq = at(yy=y + 1), at(yy=y + 3)
    zn, zq = at(zz=z + 1), at(zz=z + 7)
    pending = []

    def go(ref, index, ssem, rsem, k, dev):
        copy = send(ref.at[index], ref.at[index], ssem.at[k], rsem.at[k], dev)
        pending.append(copy)
        return copy

    low, high = pl.ds(0, 256), pl.ds(256, 256)
    offsets = (0, 3, 1, 2)

    class Spread:
        def __init__(self, ref, place, near, far, ssem, rsem):
            self.ref, self.place, self.near, self.far = ref, place, near, far
            self.sems, self.sent = (ssem, rsem), {}

        def go(self, k, d1, d2, dev, lanes=None):
            index = (rows(self.place(d1, d2)),) + (() if lanes is None else (lanes,))
            self.sent[k] = go(self.ref, index, *self.sems, k, dev)

        def arrived(self, *keys):
            for k in keys:
                self.sent[k].wait_recv()

        def second(self, j):
            for side in range(2):
                self.go(4 + 4 * side + j, offsets[j], 0, self.far[side])

        def start(self):
            self.go(0, 0, 0, self.near[0])
            self.go(1, 0, 0, self.near[1])
            self.second(0)

        def hop(self, k):
            if k == 1:
                self.arrived(0)
                self.go(2, 3, 0, self.near[0], low)
                self.arrived(1)
                self.go(3, 1, 0, self.near[1], high)
                self.second(1)
                self.second(2)
                self.arrived(4, 8)
                self.go(12, 0, 3, self.far[0])
            elif k == 2:
                self.arrived(2, 3)
                self.second(3)
                self.go(15, 2, 0, self.far[2])
                self.arrived(5, 9)
                self.go(13, 3, 1, self.far[1])
                self.arrived(6, 10)
                self.go(14, 1, 1, self.far[1])
                self.arrived(12)
            else:
                self.arrived(7, 11, 13, 14, 15)

    half_a = Spread(
        xpa, lambda d1, d2: lax.rem(y + d2, 4) * 4 + lax.rem(x + d1, 4), (xn, xq), (yn, yq, at(yy=y + 2)), a_send, a_recv
    )
    half_b = Spread(
        xpb, lambda d1, d2: lax.rem(y + d1, 4) * 4 + lax.rem(x + d2, 4), (yn, yq), (xn, xq, at(xx=x + 2)), b_send, b_recv
    )
    ring_sent = {}
    parts = (pl.ds(0, 512), pl.ds(512, 512))

    def ring(step, side, h, dist, dev):
        owner = lax.rem(z + (8 - dist if side == 0 else dist), 8)
        key = step * 4 + side * 2 + h
        ring_sent[key] = go(xl, (c, rows(owner), parts[h]), z_send, z_recv, key, dev)

    def ring_hop(k, h):
        for side in range(2):
            ring_sent[(k - 1) * 4 + side * 2 + h].wait_recv()
            if k < 3:
                ring(k, side, h, k, (zn, zq)[side])
            if k == 2 and side == h:
                ring(3, side, h, k, (at(zz=z + 2), at(zz=z + 6))[side])
        if k == 3 and h == 1:
            for key in (12, 15):
                ring_sent[key].wait_recv()

    half_a.start()
    half_b.start()
    for h in range(2):
        for side in range(2):
            ring(0, side, h, 0, (zn, zq)[side])
    for k in range(15):
        send(side_ref, side_p.at[me_p], sp_sems.at[0], sp_sems.at[1], plane_peers[k])
    for k in range(7):
        send(side_ref, side_l.at[z], sl_sems.at[0], sl_sems.at[1], line_same[k])
    side_p[me_p] = side_ref[...]
    side_l[z] = side_ref[...]

    def hop(k):
        ring_hop(k, 0)
        half_a.hop(k)
        ring_hop(k, 1)
        half_b.hop(k)

    near = {0: ((0, 0),), 1: ((0, 1), (0, 3), (1, 0), (3, 0)),
            2: ((2, 0), (0, 2), (1, 1), (1, 3), (3, 1), (3, 3)),
            3: ((2, 1), (2, 3), (1, 2), (3, 2), (2, 2))}

    def plane_slots(k):
        return [lax.rem(y + dy, 4) * 4 + lax.rem(x + dx, 4) for dx, dy in near[k]]

    def line_slots(k):
        return [lax.rem(z + d, 8) for d in {0: (0,), 1: (1, 7), 2: (2, 6), 3: (3, 5, 4)}[k]]

    def many(ref, count, sems, which):
        view = ref.at[pl.ds(0, count)]
        pltpu.make_async_copy(view, view, sems.at[which]).wait()

    def columns():
        many(side_p, 15, sp_sems, 1)
        many(side_l, 7, sl_sems, 1)
        side_rows[...] = jnp.zeros_like(side_rows)
        side_rows[0:16, :] = side_p[:, 0, :]
        side_rows[16:32, :] = side_p[:, 1, :]
        side_rows[32:40, :] = side_l[:, 0, :]
        side_rows[40:48, :] = side_l[:, 1, :]
        turned = side_rows[...].T
        lane = lax.broadcasted_iota(jnp.int32, (CHUNK, 128), 1)
        for s in range(16):
            place = pl.ds(s * CHUNK, CHUNK)
            wcol_p[place, :] = jnp.broadcast_to(turned[0:CHUNK, s : s + 1], (CHUNK, 128))
            tcol_p[place, :] = jnp.where(lane == 0, turned[0:CHUNK, 16 + s : 17 + s], 0.0)
        for s in range(8):
            place = pl.ds(s * CHUNK, CHUNK)
            wcol_l[place, :] = jnp.broadcast_to(turned[0:CHUNK, 32 + s : 33 + s], (CHUNK, 128))
            tcol_l[place, :] = jnp.where(lane == 0, turned[0:CHUNK, 40 + s : 41 + s], 0.0)

    def wide(n):
        return pl.ds(pl.multiple_of(n * WIDE, WIDE), WIDE)

    def batch(line, plane, middle):
        chunks = [(xl, hl, ol, il, q_l, wcol_l, tcol_l, slot) for slot in line]
        chunks += [(None, hp, op, ip, q_p, wcol_p, tcol_p, slot) for slot in plane]
        size = len(chunks) * CHUNK
        span = pl.ds(0, size)
        for k, chunk in enumerate(chunks):
            to, at_slot = pl.ds(k * CHUNK, CHUNK), rows(chunk[-1])
            if chunk[0] is None:
                xs[to, 0:512] = xpa[at_slot, :]
                xs[to, 512:1024] = xpb[at_slot, :]
            else:
                xs[to, :] = xl[c, at_slot, :]

        def put(which, lanes, value):
            for k, chunk in enumerate(chunks):
                piece = value[k * CHUNK : (k + 1) * CHUNK]
                if chunk[0] is None:
                    chunk[which][rows(chunk[-1]), lanes] = piece
                else:
                    chunk[which][c, rows(chunk[-1]), lanes] = piece

        for n in range(4):
            lanes = pl.ds(n * WIDE, WIDE)
            pre = dot(xs[span, :], w1[:, lanes])
            s = sigmoid(pre)
            value = (pre * s).astype(BF16)
            hs[span, lanes] = value
            put(1, lanes, value)
            slope[span, lanes] = s * (1.0 + pre * (1.0 - s))
        middle()
        for k, chunk in enumerate(chunks):
            to, at_slot = pl.ds(k * CHUNK, CHUNK), rows(chunk[-1])
            wcol[to, :] = chunk[5][at_slot, :]
        for n in range(4):
            lanes = pl.ds(n * WIDE, WIDE)
            pre = dot(hs[span, :], w2[:, lanes])
            s = sigmoid(pre)
            gain = gain_row[0:1, lanes]
            silu = pre * s * gain
            silu = silu[:, 0:128] + silu[:, 128:256]
            if n == 0:
                sig[span, :] = silu
            else:
                sig[span, :] += silu
            value = (twice(wcol[span, :]) * (s * (1.0 + pre * (1.0 - s))) * gain).astype(BF16)
            os[span, lanes] = value
            put(2, lanes, value)
        for n in range(4):
            lanes = pl.ds(n * WIDE, WIDE)
            back = dot_nt(os[span, :], w2[lanes, :])
            put(3, lanes, (back * slope[span, lanes]).astype(BF16))
        for k, chunk in enumerate(chunks):
            to, at_slot = pl.ds(k * CHUNK, CHUNK), rows(chunk[-1])
            chunk[4][at_slot, :] = sig[to, :] * wcol[to, :] - chunk[6][at_slot, :]
    sub = lax.broadcasted_iota(jnp.int32, (8, 128), 0)

    def packed(lines, first=0):
        value = jnp.zeros((8, 128), F32)
        for k, line in enumerate(lines):
            value = jnp.where(sub == first + k, line, value)
        return value

    partner = at(cc=1 - c)
    core_copies = []

    def share(view):
        k = len(core_copies)
        core_copies.append(send(view, view, core_send.at[k], core_recv.at[k], partner))

    def share_all(line):
        for slot in line:
            for ref in (xl, hl, ol, il):
                share(ref.at[c, rows(slot)])

    loads[7].wait()
    hop(1)
    loads[8].wait()
    line = line_slots(0) + line_slots(1)
    batch(line, plane_slots(0) + plane_slots(1), columns)
    for k in (2, 3):
        hop(k)
        share_all(line)
        line = line_slots(k)
        batch(line, plane_slots(k), lambda: None)
    share_all(line)

    def as_lines(ref, count):
        return [jnp.sum(ref[pl.ds(b * 128, 128), :].T, axis=0, keepdims=True) for b in range(count)]

    half_r[c] = packed(as_lines(q_l, 3), c * 3)
    share(half_r.at[c])
    r0p = packed(as_lines(q_p, 6))

    def gram(which):
        def block(n, carry):
            place = wide(n)
            one = dot_nt(xl[which, :, 0:512], xpa[place, :]) + dot_nt(xl[which, :, 512:1024], xpb[place, :])
            value = one * dot_nt(il[which], ip[place, :])
            value = value + dot_nt(hl[which], hp[place, :]) * dot_nt(ol[which], op[place, :])
            kern[which, :, place] = value
            return carry

        lax.fori_loop(0, 3, block, 0, unroll=3)

    gram(c)
    for copy in core_copies:
        copy.wait_recv()
    r0l = half_r[0] + half_r[1]
    gram(1 - c)

    def products(dp, dl):
        lines_l, sums = [], [None] * 6
        for b in range(6):
            part = kern.at[b // 3, pl.ds((b % 3) * 128, 128)]
            if dl is not None:
                col = jnp.broadcast_to(dl[b : b + 1, :], (128, 128)).T
            acc = None
            for t in range(6):
                tile = part[:, t * 128 : (t + 1) * 128]
                term = tile * dp[t : t + 1, :]
                acc = term if acc is None else acc + term
                if dl is not None:
                    down = jnp.sum((tile * col).reshape(16, 8, 128), axis=0)
                    sums[t] = down if sums[t] is None else sums[t] + down
            lines_l.append(jnp.sum(acc.T, axis=0, keepdims=True))
        lines_p = [jnp.sum(s, axis=0, keepdims=True) for s in sums] if dl is not None else []
        return lines_p, packed(lines_l)

    def start_plane(k, value):
        plane_buf[k, me_p] = value
        for peer in plane_peers:
            send(plane_buf.at[k, me_p], plane_buf.at[k, me_p], plane_sems.at[k, 0], plane_sems.at[k, 1], peer)

    def start_line(k, value):
        line_buf[k, me_l] = value
        for peer in line_peers:
            send(line_buf.at[k, me_l], line_buf.at[k, me_l], line_sems.at[k, 0], line_sems.at[k, 1], peer)

    def end_plane(k):
        many(plane_buf.at[k], 15, plane_sems.at[k], 1)
        return jnp.sum(plane_buf[k], axis=0)

    def end_line(k):
        many(line_buf.at[k], 15, line_sems.at[k], 1)
        return jnp.sum(line_buf[k], axis=0)

    def scalars(m, n):
        return [jnp.zeros((1, 128), F32)] * 6 + [jnp.broadcast_to(m, (1, 128)), jnp.broadcast_to(n, (1, 128))]

    def summed(which, at_term, vectors):
        turned_ref, right = ((x_t, il), (h_t, ol))[which]
        left = jnp.concatenate(
            [turned_ref[pl.ds(pl.multiple_of(c * 32 + 64 * k, 32), 32), :] for k in range(2)], axis=0
        )
        basis = [jnp.concatenate([vector[b : b + 1, :] for b in range(6)], axis=1) for vector in vectors]
        scaled = [left * across for across in basis]
        coarse = [value.astype(BF16) for value in scaled]
        fine = [(value - part.astype(F32)).astype(BF16) for value, part in zip(scaled, coarse)]
        stack = jnp.concatenate(coarse + fine, axis=0)
        half = 64 * len(vectors)
        for n in range(4):
            lanes = pl.ds(n * WIDE, WIDE)
            found = dot(stack, right[:, :, lanes].reshape(SET, WIDE))
            for k in range(len(vectors)):
                near, far = found[64 * k : 64 * k + 64], found[half + 64 * k : half + 64 * k + 64]
                terms[which, at_term + k, :, lanes] = near + far

    sub_wide = lax.broadcasted_iota(jnp.int32, (8, 1024), 0)

    def stage(slot, one, two):
        for e in range(8):
            f, s = one[8 * e : 8 * e + 8], two[8 * e : 8 * e + 8]
            out_send[slot, 2 * e] = jnp.where(sub_wide < 4, f, pltpu.roll(s, 4, 0)).astype(BF16)
            out_send[slot, 2 * e + 1] = jnp.where(sub_wide < 4, pltpu.roll(f, 4, 0), s).astype(BF16)
        out_recv[slot, me_p] = out_send[slot, me_p]

    def give(slot):
        for k, peer in zip(plane_order, plane_peers):
            dest = lax.rem(y + k // 4, 4) * 4 + lax.rem(x + k % 4, 4)
            send(out_send.at[slot, dest], out_recv.at[slot, me_p], out_sems.at[slot, 0], out_sems.at[slot, 1], peer)

    def whole(factor):
        return jnp.concatenate([factor] * 8, axis=1)

    lines_p, part_l = products(r0p, r0l)
    start_line(0, part_l)
    start_plane(0, packed(lines_p))
    mine = pl.ds(pl.multiple_of(z * 128, 128), 128)
    for b in range(6):
        place = pl.ds((b % 3) * 128, 128)
        x_t[:, b * 128 : (b + 1) * 128] = xl[b // 3, place, mine].astype(F32).T
        h_t[:, b * 128 : (b + 1) * 128] = hl[b // 3, place, mine].astype(F32).T
    summed(0, 0, (r0l,))
    summed(1, 0, (r0l,))
    stage(0, terms[0, 0], terms[1, 0])
    w0p = end_plane(0) + DAMP * r0p
    w0l = end_line(0) + DAMP * r0l
    m0, m1 = total_of(r0l * r0l), total_of(r0l * w0l)
    lines_p, part_l = products(w0p, w0l)
    start_line(1, part_l)
    first_lanes = lax.broadcasted_iota(jnp.int32, (1, 128), 1) < 64
    start_plane(1, packed(lines_p + [
        jnp.where(first_lanes, m0, total_of(w0l * w0l)), jnp.broadcast_to(m1, (1, 128))
    ]))
    give(0)
    got = end_plane(1)
    u0p = got + DAMP * w0p
    u0l = end_line(1) + DAMP * w0l
    rr0, rw0 = jnp.broadcast_to(got[6:7, 0:1], (1, 128)), got[7:8, :]
    w0w0 = jnp.broadcast_to(got[6:7, 64:65], (1, 128))
    al0 = rr0 / rw0
    r1l, w1l = r0l - al0 * w0l, w0l - al0 * u0l
    w1p = w0p - al0 * u0p
    m0, m1 = total_of(r1l * r1l), total_of(r1l * w1l)
    near0 = al0 * al0 * w0w0 / rr0 - 1.0
    e1l = r1l + near0 * r0l
    start_plane(2, packed([
        jnp.broadcast_to(value, (1, 128)) for value in (m0, m1, total_of(w1l * w1l), total_of(w1l * w0l))
    ]))
    _, part_l = products(w1p, None)
    start_line(2, part_l)
    summed(0, 1, (e1l, w1l, w0l))
    summed(1, 1, (e1l, w1l, w0l))
    stage(1, terms[0, 1], terms[1, 1])
    give(1)
    got = end_plane(2)
    u1l = end_line(2) + DAMP * w1l
    rr1, rw1, w1w1, w1w0 = [got[k : k + 1, :] for k in range(4)]
    be0 = rr1 / rr0
    al1 = rr1 / (rw1 - be0 * rr1 / al0)
    r2l = r1l - al1 * (w1l + be0 * w0l)
    w2l = w1l - al1 * (u1l + be0 * u0l)
    m0, m1 = total_of(r2l * r2l), total_of(r2l * w2l)
    start_plane(3, packed(scalars(m0, m1)))
    near1 = al1 * al1 * (w1w1 + 2.0 * be0 * w1w0 + be0 * be0 * w0w0) / rr1 - 1.0
    left_over = be0 - near0
    stage(2, *[
        whole(1.0 + near1) * terms[k, 1] + whole(near1 * left_over - near0) * terms[k, 0]
        - whole(al1) * (terms[k, 2] + whole(be0) * terms[k, 3])
        for k in range(2)
    ])
    give(2)
    got = end_plane(3)
    rr2, rw2 = got[6:7, :], got[7:8, :]
    be1 = rr2 / rr1
    al2 = rr2 / (rw2 - be1 * rr2 / al1)
    both = al1 + al2 * (be1 - near1)
    result = None
    for slot, factor in enumerate((al0 + both * left_over, both, al2)):
        many(out_recv.at[slot], 15, out_sems.at[slot], 1)
        term = jnp.sum(out_recv[slot].astype(F32), axis=0) * whole(-LEARN * factor)
        result = term if result is None else result + term
    out_ref[:, 0:1024] = result[0:4]
    out_ref[:, 1024:2048] = result[4:8]

    for copy in pending + core_copies:
        copy.wait_send()
    many(side_p, 15, sp_sems, 0)
    many(side_l, 7, sl_sems, 0)
    for k in range(4):
        many(plane_buf.at[k], 15, plane_sems.at[k], 0)
    for k in range(3):
        many(line_buf.at[k], 15, line_sems.at[k], 0)
    for slot in range(3):
        many(out_send.at[slot], 15, out_sems.at[slot], 0)


def shards(inputs, first_weight, second_weight, readout, target, counts, views):
    vmem = pl.BlockSpec(memory_space=pltpu.VMEM)
    hbm = pl.BlockSpec(memory_space=pltpu.HBM)
    dma = pltpu.SemaphoreType.DMA
    return pl.pallas_call(
        step_kernel,
        out_shape=jax.ShapeDtypeStruct((4, 2048), F32),
        in_specs=[hbm] * 7,
        out_specs=vmem,
        scratch_shapes=[
            pltpu.VMEM((8, 128), BF16), pltpu.VMEM((1, CHUNK), F32),
            pltpu.VMEM((1, CHUNK), jnp.int32), pltpu.VMEM((1, CHUNK), jnp.int32),
            pltpu.VMEM((1, 1024), F32), pltpu.VMEM((2, 128), F32),
            pltpu.VMEM((1024, 1024), BF16), pltpu.VMEM((1024, 1024), BF16),
            pltpu.VMEM((SET, 512), BF16), pltpu.VMEM((SET, 512), BF16),
            pltpu.VMEM((SET, 1024), BF16), pltpu.VMEM((SET, 1024), BF16), pltpu.VMEM((SET, 1024), BF16),
            pltpu.VMEM((2, HALF, 1024), BF16), pltpu.VMEM((2, HALF, 1024), BF16),
            pltpu.VMEM((2, HALF, 1024), BF16), pltpu.VMEM((2, HALF, 1024), BF16),
            pltpu.VMEM((HALF, 1024), BF16), pltpu.VMEM((HALF, 1024), BF16), pltpu.VMEM((HALF, 1024), BF16),
            pltpu.VMEM((HALF, 1024), F32), pltpu.VMEM((HALF, 128), F32),
            pltpu.VMEM((2, HALF, SET), F32),
            pltpu.VMEM((16, 2, 128), F32), pltpu.VMEM((8, 2, 128), F32), pltpu.VMEM((128, 128), F32),
            pltpu.VMEM((SET, 128), F32), pltpu.VMEM((SET, 128), F32),
            pltpu.VMEM((HALF, 128), F32), pltpu.VMEM((HALF, 128), F32), pltpu.VMEM((HALF, 128), F32),
            pltpu.VMEM((SET, 128), F32), pltpu.VMEM((HALF, 128), F32),
            pltpu.VMEM((2, 8, 128), F32), pltpu.VMEM((128, SET), F32), pltpu.VMEM((128, SET), F32),
            pltpu.VMEM((2, 4, 64, 1024), F32), pltpu.VMEM((4, 16, 8, 128), F32), pltpu.VMEM((3, 16, 8, 128), F32),
            pltpu.VMEM((3, 16, 8, 1024), BF16), pltpu.VMEM((3, 16, 8, 1024), BF16),
            dma((9,)), dma((16,)), dma((16,)), dma((16,)), dma((16,)), dma((16,)), dma((16,)),
            dma((33,)), dma((33,)), dma((2,)), dma((2,)), dma((4, 2)), dma((3, 2)), dma((3, 2)),
        ],
        compiler_params=pltpu.CompilerParams(
            collective_id=0, has_side_effects=True, vmem_limit_bytes=56 * 1024 * 1024
        ),
    )(
        inputs, first_weight, second_weight, readout.reshape(8, 128),
        target.reshape(1, CHUNK), counts.reshape(1, CHUNK), views.reshape(1, CHUNK),
    )


def solution(mesh):
    split = Mesh(mesh.devices.reshape(8, 2, 2, 2, 4), AXES)
    return jax.shard_map(
        shards,
        mesh=split,
        in_specs=(P(AXES, None), P(), P(), P(), P(AXES), P(AXES), P(AXES)),
        out_specs=P(AXES, None),
        check_vma=False,
    )
```
